32 devices in a mesh: rows: 8 (over z, y), rep: 4 (over x, core).
Axes of the slice: x: 2, y: 2, z: 4, core: 2. Of those that a mesh axis runs over, the one named last changes fastest.
Arguments:
- event_slots: int32 [32, 128], P(('rows', 'rep')), may hold values from 0 to 143, as said below
- fetch_rows: int32 [32, 16], P(('rows', 'rep')), may hold values from 0 to 255, as said below
- fetch_counts: int32 [32, 8], P(('rows', 'rep')), may hold values from 1 to 2, as said below
- hot_table: float32 [128, 512], replicated, may hold values from -6 to 6
- hot_accum: float32 [128], replicated, may hold values from 0.05 to 2
- cold_table: float32 [2048, 512], P('rows'), may hold values from -6 to 6
- cold_accum: float32 [2048], P('rows'), may hold values from 0.05 to 2
- ln_gain: float32 [512], replicated, may hold values from 0.1 to 1.9
- ln_bias: float32 [512], replicated, may hold values from -3 to 3
- w_in: bfloat16 [512, 2048], replicated, may hold values from -0.25 to 0.25
- w_out: bfloat16 [512, 512], replicated, may hold values from -0.25 to 0.25
- out_grad: bfloat16 [4096, 512], P(('rows', 'rep')), may hold values from -6 to 6
Outputs:
- new_hot_table: float32 [128, 512], replicated
- new_hot_accum: float32 [128], replicated
- new_cold_table: float32 [2048, 512], P('rows')
- new_cold_accum: float32 [2048], P('rows')
The draws below stay inside these ranges and needn't reach their ends.
Inputs may be any that keep to these rules, and one draw needn't show every extreme that they name: `event_slots`: rows of the lookup buffer: the 128 hot rows, then 2 slots for each of the 8 owners; an event names slot k of owner j only if k is below that device's fetch_counts for j. `fetch_rows`: rows local to the owner's shard, distinct within one owner's 2 slots of one device; slots at or past the count are padding. `fetch_counts`: some owner is asked for 2 rows by every device.
All inputs are finite; a program needn't handle non-finite values.
Results may differ from the reference program's by a relative error of at most 0.0065.
Values sent between devices are 32-bit elements; how exact they have to be, the bound alone decides.
No kernel may reach another device: no remote copies, remote signals or barrier semaphores. Data moves between devices by JAX's collectives and lax.ppermute only.
A program may use at most 64 MiB of HBM per device.

```python
import math
import jax
import jax.numpy as jnp
from jax import lax

D = 512
HEADS = 4
HEAD = 128
SEQ_LEN = 128
ROWS_DEV = 256
HOT_ROWS = 128
SLOT = 2
TOKENS = 4096
COLD_ROWS = 2048
N_ROWS = 8
DEVICES = 32


def owner_counts(key):
    base = jax.random.fold_in(key, 11)
    counts = jax.random.randint(jax.random.fold_in(base, 1), (DEVICES, N_ROWS), 1, SLOT + 1)
    full_owner = jax.random.randint(jax.random.fold_in(base, 2), (), 0, N_ROWS)
    column = jnp.arange(N_ROWS, dtype=jnp.int32)[None, :] == full_owner
    return jnp.where(column, SLOT, counts).astype(jnp.int32)


def draw_fetch_counts(key, part):
    return owner_counts(key)


def draw_fetch_rows(key, part):
    stride = ROWS_DEV // SLOT
    offsets = jax.random.randint(jax.random.fold_in(key, 23), (DEVICES, N_ROWS, SLOT), 0, stride)
    picked = offsets + jnp.arange(SLOT, dtype=jnp.int32)[None, None, :] * stride
    return picked.reshape(DEVICES, N_ROWS * SLOT).astype(jnp.int32)


def draw_event_slots(key, part):
    counts = owner_counts(key)
    shape = (DEVICES, SEQ_LEN)
    hot_pick = jax.random.randint(jax.random.fold_in(key, 31), shape, 0, HOT_ROWS)
    owner = jax.random.randint(jax.random.fold_in(key, 32), shape, 0, N_ROWS)
    limit = jnp.take_along_axis(counts, owner, axis=1)
    within = jax.random.randint(jax.random.fold_in(key, 33), shape, 0, limit)
    cold_pick = HOT_ROWS + owner * SLOT + within
    coin = jax.random.randint(jax.random.fold_in(key, 34), shape, 0, 2)
    return jnp.where(coin == 0, hot_pick, cold_pick).astype(jnp.int32)


def levels(own_key, shape, cuts, low, high):
    def one(dim, blocks):
        steps = jax.random.uniform(jax.random.fold_in(jax.random.fold_in(own_key, 6), dim), (blocks,), jnp.float32, low / len(cuts), high / len(cuts))
        return jnp.repeat(jnp.exp(steps), shape[dim] // blocks).reshape((-1,) + (1,) * (len(shape) - dim - 1))

    loudness = one(*cuts[0])
    for cut in cuts[1:]:
        loudness = loudness * one(*cut)
    return loudness


def gaussian(rng, shape, width, reach, cuts=(), held_as=jnp.bfloat16):
    values = width * jax.random.normal(rng, shape, jnp.float32)
    if cuts:
        values = values * levels(rng, shape, cuts, -0.22, 0.18)
    return jnp.clip(values, -reach, reach).astype(held_as)


def setup_inputs(seed: int = 0) -> dict:
    key_list = jax.random.split(jax.random.key(seed), 13)
    return {
        "event_slots": draw_event_slots(jax.random.fold_in(key_list[12], 71), 0),
        "fetch_rows": draw_fetch_rows(jax.random.fold_in(key_list[12], 71), 0),
        "fetch_counts": draw_fetch_counts(jax.random.fold_in(key_list[12], 71), 0),
        "hot_table": gaussian(key_list[3], (HOT_ROWS, D), 1.0, 6.0, (), jnp.float32),
        "hot_accum": jnp.clip(jnp.exp(jax.random.uniform(key_list[4], (HOT_ROWS,), jnp.float32, math.log(0.05), math.log(2.0))), 0.05, 2.0),
        "cold_table": gaussian(key_list[5], (COLD_ROWS, D), 1.0, 6.0, ((0, 8),), jnp.float32),
        "cold_accum": jnp.clip(jnp.exp(math.log(2.0) - 3.6888794 * jax.random.uniform(key_list[6], (COLD_ROWS,), jnp.float32) ** levels(key_list[6], (COLD_ROWS,), ((0, 8),), -0.2, 0.2)), 0.05, 2.0),
        "ln_gain": jnp.clip(1.0 + 0.18 * jax.random.normal(key_list[7], (D,), jnp.float32), 0.1, 1.9),
        "ln_bias": gaussian(key_list[8], (D,), 0.5, 3.0, (), jnp.float32),
        "w_in": gaussian(key_list[9], (D, 4 * HEADS * HEAD), D ** -0.5, 0.25),
        "w_out": gaussian(key_list[10], (HEADS * HEAD, D), (HEADS * HEAD) ** -0.5, 0.25),
        "out_grad": gaussian(key_list[11], (TOKENS, D), 1.0, 6.0, ((0, 32),)),
    }


STEP_RATE = 0.5

def hstu_layer(looked_up, ln_gain, ln_bias, w_in, w_out):
    seq_rows = looked_up.shape[0]
    inner = w_out.shape[0]
    n_heads = inner // HEAD
    row_mean = lax.optimization_barrier(jnp.mean(looked_up, axis=1, keepdims=True))
    centered = looked_up - row_mean
    row_var = lax.optimization_barrier(jnp.mean(centered * centered, axis=1, keepdims=True))
    normed = (centered * lax.rsqrt(row_var + 1e-05) * ln_gain + ln_bias).astype(jnp.bfloat16)
    projected = jax.nn.silu(jnp.dot(normed, w_in, preferred_element_type=jnp.float32)).astype(jnp.bfloat16)
    gates_u, values_v, queries, keys_k = jnp.split(projected, 4, axis=1)
    head_shape = (seq_rows, n_heads, HEAD)
    scores = jnp.einsum('qhd,khd->hqk', queries.reshape(head_shape).astype(jnp.float32), keys_k.reshape(head_shape).astype(jnp.float32)) * HEAD ** (-0.5)
    causal = (lax.broadcasted_iota(jnp.int32, (seq_rows, seq_rows), 0) >= lax.broadcasted_iota(jnp.int32, (seq_rows, seq_rows), 1)).astype(jnp.float32)
    attention = (jax.nn.silu(scores) * causal * (1.0 / seq_rows)).astype(jnp.bfloat16)
    mixed_val = jnp.einsum('hqk,khd->qhd', attention.astype(jnp.float32), values_v.reshape(head_shape).astype(jnp.float32)).reshape(seq_rows, inner)
    mixed_mean = lax.optimization_barrier(jnp.mean(mixed_val, axis=1, keepdims=True))
    mixed_cent = mixed_val - mixed_mean
    mixed_var = lax.optimization_barrier(jnp.mean(mixed_cent * mixed_cent, axis=1, keepdims=True))
    gated_val = (mixed_cent * lax.rsqrt(mixed_var + 1e-06) * gates_u.astype(jnp.float32)).astype(jnp.bfloat16)
    layer_out = looked_up + jnp.dot(gated_val, w_out, preferred_element_type=jnp.float32)
    return layer_out.astype(jnp.bfloat16)

def adagrad(table_rows, accum_rows, grad_rows):
    new_accum = accum_rows + lax.optimization_barrier(jnp.mean(grad_rows * grad_rows, axis=1))
    return (table_rows - STEP_RATE * grad_rows * lax.rsqrt(new_accum)[:, None], new_accum)

def reference(event_slots, fetch_rows, fetch_counts, hot_table, hot_accum, cold_table, cold_accum, ln_gain, ln_bias, w_in, w_out, out_grad):
    device_count = event_slots.shape[0]
    seq_rows = event_slots.shape[1]
    feature_width = hot_table.shape[1]
    hot_rows = hot_table.shape[0]
    per_owner = fetch_rows.shape[1] // N_ROWS
    rows_shard = cold_table.shape[0] // N_ROWS
    owner_base = (jnp.arange(N_ROWS, dtype=jnp.int32) * rows_shard)[:, None]
    cotangents = out_grad.reshape(device_count, seq_rows, feature_width)

    def forward_for(ln_g, ln_b):

        def forward(looked_up):
            return hstu_layer(looked_up, ln_g, ln_b, w_in, w_out)
        return forward
    forward = forward_for(ln_gain, ln_bias)

    def one_device(running, inputs):
        hot_sum, cold_sum = running
        event_rows, wanted, counts, cotangent = inputs
        global_rows = (wanted.reshape(N_ROWS, per_owner) + owner_base).reshape(-1).astype(jnp.int32)
        live_mask = (jnp.arange(per_owner, dtype=jnp.int32)[None, :] < counts[:, None]).reshape(-1, 1).astype(jnp.float32)
        fetched = cold_table[global_rows] * live_mask
        buffer = jnp.concatenate([hot_table, fetched], axis=0)
        looked_up = buffer[event_rows]
        _, backward = jax.vjp(forward, looked_up)
        d_lookup, = backward(cotangent)
        buffer_grad = jax.ops.segment_sum(d_lookup, event_rows, num_segments=hot_rows + N_ROWS * per_owner)
        hot_sum = hot_sum + buffer_grad[:hot_rows]
        cold_sum = cold_sum.at[global_rows].add(buffer_grad[hot_rows:] * live_mask)
        return ((hot_sum, cold_sum), None)
    start = (jnp.zeros(hot_table.shape, jnp.float32), jnp.zeros(cold_table.shape, jnp.float32))
    (hot_grad, cold_grad), _ = lax.scan(one_device, start, (event_slots, fetch_rows, fetch_counts, cotangents))
    new_hot_table, new_hot_accum = adagrad(hot_table, hot_accum, hot_grad)
    new_cold_table, new_cold_accum = adagrad(cold_table, cold_accum, cold_grad)
    return (new_hot_table, new_hot_accum, new_cold_table, new_cold_accum)
```

```python
import functools

import jax
import jax.numpy as jnp
from jax import lax
from jax.experimental import pallas as pl
from jax.experimental.pallas import tpu as pltpu
from jax.sharding import PartitionSpec as P

HEAD = 128
STEP_RATE = 0.5
LANES = 128
SUBLANES = 8
ALL = ("rows", "rep")
F32 = jnp.float32
BF16 = jnp.bfloat16

VMEM = pl.BlockSpec(memory_space=pltpu.VMEM)
SMEM = pl.BlockSpec(memory_space=pltpu.SMEM)


def params(mib=24):
    return pltpu.CompilerParams(vmem_limit_bytes=mib << 20)


def dot(a, b, dims, precision=None):
    return lax.dot_general(
        a, b, (dims, ((), ())), preferred_element_type=F32, precision=precision
    )


NN = ((1,), (0,))
NT = ((1,), (1,))
TN = ((0,), (0,))


def loop(count, body):
    for i in range(count):
        body(i)


def gather_kernel(place_ref, asked_ref, table_ref, out_ref, rows_scr, *, n_rows, n_rep, slot):
    j = place_ref[0]
    p = place_ref[1]
    per_row = asked_ref.shape[1]
    shard = table_ref.shape[0]
    width = table_ref.shape[1]
    chunks = width // LANES

    def take(r):
        rows_scr[pl.ds(r * per_row, per_row), :] = asked_ref[r * n_rep + p]

    loop(n_rows, take)
    asked = rows_scr[...].reshape(n_rows, per_row * LANES) if per_row == 1 else None
    table = table_ref[...]
    for k in range(slot):
        at = j * slot + k
        if per_row == 1:
            lane = lax.broadcasted_iota(jnp.int32, (n_rows, LANES), 1)
            col = jnp.sum(jnp.where(lane == at, asked, 0), axis=1, keepdims=True)
        else:
            flat = rows_scr[...].reshape(n_rows, per_row, LANES)
            pos = lax.broadcasted_iota(jnp.int32, flat.shape, 1) * LANES + lax.broadcasted_iota(
                jnp.int32, flat.shape, 2
            )
            col = jnp.sum(jnp.sum(jnp.where(pos == at, flat, 0), axis=1), axis=1, keepdims=True)
        pick = (lax.broadcasted_iota(jnp.int32, (n_rows, shard), 1) == col).astype(F32)
        rows = dot(pick, table, NN, lax.Precision.HIGHEST)
        for c in range(chunks):
            out_ref[:, k * chunks + c, :] = rows[:, c * LANES : (c + 1) * LANES]


def layer_kernel(
    event_ref,
    count_ref,
    hot_ref,
    fetched_ref,
    gain_ref,
    bias_ref,
    w_in_ref,
    w_out_ref,
    grad_ref,
    out_ref,
    x_scr,
    *,
    n_dev,
    n_rep,
    slot,
):
    hot_rows, width = hot_ref.shape
    n_owner = fetched_ref.shape[0]
    chunks = width // LANES
    slots = x_scr.shape[0]
    seq = grad_ref.shape[0]
    inner = w_out_ref.shape[0]
    heads = inner // HEAD

    x_scr[0:hot_rows, :] = hot_ref[...]

    def place(j):
        for k in range(slot):
            live = (k < count_ref[0, j]).astype(F32)
            for c in range(chunks):
                x_scr[pl.ds(hot_rows + j * slot + k, 1), c * LANES : (c + 1) * LANES] = (
                    fetched_ref[j, pl.ds(k * chunks + c, 1), :] * live
                )

    loop(n_owner, place)

    x = x_scr[...]
    mean = jnp.mean(x, axis=1, keepdims=True)
    cent = x - mean
    var = jnp.mean(cent * cent, axis=1, keepdims=True)
    rstd = lax.rsqrt(var + 1e-05)
    xhat = cent * rstd
    gain = gain_ref[...]
    normed = (xhat * gain + bias_ref[...]).astype(BF16)

    pre = dot(normed, w_in_ref[...], NN)
    sig = jax.nn.sigmoid(pre)
    proj = (pre * sig).astype(BF16)
    dsilu = sig * (1.0 + pre * (1.0 - sig))

    event_row = event_ref[...]
    scatter = (
        lax.broadcasted_iota(jnp.int32, (slots, seq), 0) == jnp.broadcast_to(event_row, (slots, seq))
    ).astype(F32)
    scatter_b = scatter.astype(BF16)

    proj_ev = dot(scatter_b, proj, TN).astype(BF16)
    gates = proj_ev[:, 0:inner].astype(F32)

    scale = HEAD ** (-0.5)
    causal = (
        lax.broadcasted_iota(jnp.int32, (seq, seq), 0)
        >= lax.broadcasted_iota(jnp.int32, (seq, seq), 1)
    ).astype(F32) * (1.0 / seq)

    values, queries, keys, atts, dacts, mixeds = [], [], [], [], [], []
    for h in range(heads):
        lo = h * HEAD
        v = proj_ev[:, inner + lo : inner + lo + HEAD]
        q = proj_ev[:, 2 * inner + lo : 2 * inner + lo + HEAD]
        kk = proj_ev[:, 3 * inner + lo : 3 * inner + lo + HEAD]
        s = dot(q, kk, NT) * scale
        sg = jax.nn.sigmoid(s)
        a = (s * sg * causal).astype(BF16)
        dacts.append(sg * (1.0 + s * (1.0 - sg)) * causal)
        values.append(v)
        queries.append(q)
        keys.append(kk)
        atts.append(a)
        mixeds.append(dot(a, v, NN))
    mixed = jnp.concatenate(mixeds, axis=1)
    mmean = jnp.mean(mixed, axis=1, keepdims=True)
    mcent = mixed - mmean
    mvar = jnp.mean(mcent * mcent, axis=1, keepdims=True)
    mrstd = lax.rsqrt(mvar + 1e-06)
    y = mcent * mrstd

    grad = grad_ref[...]
    d_gated = dot(grad, w_out_ref[...], NT).astype(BF16).astype(F32)
    d_gates = (d_gated * y).astype(BF16)
    d_y = d_gated * gates
    d_mixed = mrstd * (
        d_y - jnp.mean(d_y, axis=1, keepdims=True) - y * jnp.mean(d_y * y, axis=1, keepdims=True)
    )
    d_mixed = d_mixed.astype(BF16)
    d_vs, d_qs, d_ks = [], [], []
    for h in range(heads):
        dm = d_mixed[:, h * HEAD : (h + 1) * HEAD]
        d_a = dot(dm, values[h], NT).astype(BF16).astype(F32)
        d_vs.append(dot(atts[h], dm, TN).astype(BF16))
        d_s = (d_a * dacts[h] * scale).astype(BF16)
        d_qs.append(dot(d_s, keys[h], NN).astype(BF16))
        d_ks.append(dot(d_s, queries[h], TN).astype(BF16))
    d_proj = jnp.concatenate([d_gates] + d_vs + d_qs + d_ks, axis=1)

    d_slot = dot(scatter_b, d_proj, NN)
    d_pre = (d_slot * dsilu).astype(BF16)
    d_normed = dot(d_pre, w_in_ref[...], NT)
    d_hat = d_normed * gain
    d_x = rstd * (
        d_hat
        - jnp.mean(d_hat, axis=1, keepdims=True)
        - xhat * jnp.mean(d_hat * xhat, axis=1, keepdims=True)
    )
    x_scr[...] = d_x + dot(scatter_b, grad, NN)

    units = hot_rows * chunks
    share = units // n_dev
    for g in range(hot_rows // SUBLANES):
        for c in range(chunks):
            first = (g * chunks + c) * SUBLANES
            tile = x_scr[g * SUBLANES : (g + 1) * SUBLANES, c * LANES : (c + 1) * LANES]
            if share >= SUBLANES:
                out_ref[first // share, first % share : first % share + SUBLANES, :] = tile
            else:
                for i in range(SUBLANES):
                    q = first + i
                    out_ref[q // share, q % share : q % share + 1, :] = tile[i : i + 1, :]

    def send(j):
        for k in range(slot):
            live = (k < count_ref[0, j]).astype(F32)
            for c in range(chunks):
                row = (
                    x_scr[pl.ds(hot_rows + j * slot + k, 1), c * LANES : (c + 1) * LANES] * live
                )
                for p in range(n_rep):
                    out_ref[j * n_rep + p, pl.ds(share + k * chunks + c, 1), :] = row

    loop(n_owner, send)


def sum_kernel(got_ref, out_ref, *, share):
    n_dev = out_ref.shape[0]
    total = got_ref[0, 0:share, :]
    for d in range(1, n_dev):
        total = total + got_ref[d, 0:share, :]
    for d in range(n_dev):
        out_ref[d] = total


def cold_kernel(place_ref, asked_ref, got_ref, table_ref, accum_ref, new_ref, new_accum_ref, *, slot, share):
    j = place_ref[0]
    n_dev, per_row, _ = asked_ref.shape
    shard, width = table_ref.shape
    chunks = width // LANES
    asked = asked_ref[...]
    pos = lax.broadcasted_iota(jnp.int32, asked.shape, 1) * LANES + lax.broadcasted_iota(
        jnp.int32, asked.shape, 2
    )
    picks = []
    for k in range(slot):
        hit = jnp.where(pos == j * slot + k, asked, 0)
        col = jnp.sum(jnp.sum(hit, axis=1), axis=1, keepdims=True)
        picks.append(
            (lax.broadcasted_iota(jnp.int32, (n_dev, shard), 1) == col).astype(F32)
        )
    grads = []
    for c in range(chunks):
        part = None
        for k in range(slot):
            rows = got_ref[:, share + k * chunks + c, :]
            one = dot(picks[k], rows, TN, lax.Precision.HIGHEST)
            part = one if part is None else part + one
        grads.append(part)
    total = grads[0] * grads[0]
    for g in grads[1:]:
        total = total + g * g
    mean_sq = jnp.sum(total, axis=1, keepdims=True) * (1.0 / width)
    wide = jnp.transpose(jnp.broadcast_to(mean_sq, (shard, LANES)))
    accum_row = accum_ref[...]
    new_accum_ref[...] = accum_row + wide[0:1, :]
    accum_col = jnp.transpose(jnp.broadcast_to(accum_row, (LANES, shard)))[:, 0:1]
    step = lax.rsqrt(accum_col + mean_sq) * STEP_RATE
    for c in range(chunks):
        cols = slice(c * LANES, (c + 1) * LANES)
        new_ref[:, cols] = table_ref[:, cols] - grads[c] * step


def hot_kernel(got_ref, table_ref, accum_ref, new_ref, new_accum_ref, g_scr):
    n_dev, share, _ = got_ref.shape
    rows, width = table_ref.shape
    chunks = width // LANES
    for g in range(rows // SUBLANES):
        for c in range(chunks):
            first = (g * chunks + c) * SUBLANES
            at = (slice(g * SUBLANES, (g + 1) * SUBLANES), slice(c * LANES, (c + 1) * LANES))
            if share >= SUBLANES:
                g_scr[at] = got_ref[first // share, first % share : first % share + SUBLANES, :]
            else:
                for i in range(SUBLANES):
                    q = first + i
                    g_scr[g * SUBLANES + i : g * SUBLANES + i + 1, at[1]] = got_ref[
                        q // share, q % share : q % share + 1, :
                    ]
    grad = g_scr[...]
    mean_sq = jnp.mean(grad * grad, axis=1, keepdims=True)
    wide = jnp.transpose(jnp.broadcast_to(mean_sq, (rows, LANES)))
    accum_row = accum_ref[...]
    new_accum_ref[...] = accum_row + wide[0:1, :]
    accum_col = jnp.transpose(jnp.broadcast_to(accum_row, (LANES, rows)))[:, 0:1]
    new_ref[...] = table_ref[...] - STEP_RATE * grad * lax.rsqrt(accum_col + mean_sq)


def on_device(
    event_slots,
    fetch_rows,
    fetch_counts,
    hot_table,
    hot_accum,
    cold_table,
    cold_accum,
    ln_gain,
    ln_bias,
    w_in,
    w_out,
    out_grad,
):
    n_rows = lax.axis_size("rows")
    n_rep = lax.axis_size("rep")
    n_dev = n_rows * n_rep
    slot = fetch_rows.shape[1] // n_rows
    hot_rows, width = hot_table.shape
    shard = cold_table.shape[0]
    chunks = width // LANES
    share = hot_rows * chunks // n_dev
    asks = fetch_rows.shape[1]
    per_row = -(-asks // LANES)
    place = jnp.stack([lax.axis_index("rows"), lax.axis_index("rep")]).astype(jnp.int32)

    mine = jnp.pad(fetch_rows, ((0, 0), (0, per_row * LANES - asks))).reshape(1, per_row, LANES)
    asked = lax.all_to_all(
        jnp.broadcast_to(mine, (n_dev, per_row, LANES)), ALL, 0, 0, tiled=True
    )
    found = pl.pallas_call(
        functools.partial(gather_kernel, n_rows=n_rows, n_rep=n_rep, slot=slot),
        out_shape=jax.ShapeDtypeStruct((n_rows, slot * chunks, LANES), F32),
        in_specs=[SMEM, VMEM, VMEM],
        out_specs=VMEM,
        scratch_shapes=[pltpu.VMEM((n_rows * per_row, LANES), jnp.int32)],
        compiler_params=params(),
        name="gather",
    )(place, asked, cold_table)
    fetched = lax.all_to_all(found, "rows", 0, 0, tiled=True)

    slots = hot_rows + n_rows * slot
    sent = pl.pallas_call(
        functools.partial(layer_kernel, n_dev=n_dev, n_rep=n_rep, slot=slot),
        out_shape=jax.ShapeDtypeStruct((n_dev, share + slot * chunks, LANES), F32),
        in_specs=[VMEM, SMEM] + [VMEM] * 7,
        out_specs=VMEM,
        scratch_shapes=[pltpu.VMEM((slots, width), F32)],
        compiler_params=params(40),
        name="layer",
    )(
        event_slots,
        fetch_counts,
        hot_table,
        fetched,
        ln_gain.reshape(1, width),
        ln_bias.reshape(1, width),
        w_in,
        w_out,
        out_grad,
    )
    got = lax.all_to_all(sent, ALL, 0, 0, tiled=True)

    summed = pl.pallas_call(
        functools.partial(sum_kernel, share=share),
        out_shape=jax.ShapeDtypeStruct((n_dev, share, LANES), F32),
        in_specs=[VMEM],
        out_specs=VMEM,
        compiler_params=params(),
        name="sum",
    )(got)
    hot_grad = lax.all_to_all(summed, ALL, 0, 0, tiled=True)

    new_cold_table, new_cold_accum = pl.pallas_call(
        functools.partial(cold_kernel, slot=slot, share=share),
        out_shape=(
            jax.ShapeDtypeStruct((shard, width), F32),
            jax.ShapeDtypeStruct((1, shard), F32),
        ),
        in_specs=[SMEM] + [VMEM] * 4,
        out_specs=(VMEM, VMEM),
        compiler_params=params(),
        name="cold",
    )(place, asked, got, cold_table, cold_accum.reshape(1, shard))

    new_hot_table, new_hot_accum = pl.pallas_call(
        hot_kernel,
        out_shape=(
            jax.ShapeDtypeStruct((hot_rows, width), F32),
            jax.ShapeDtypeStruct((1, hot_rows), F32),
        ),
        in_specs=[VMEM] * 3,
        out_specs=(VMEM, VMEM),
        scratch_shapes=[pltpu.VMEM((hot_rows, width), F32)],
        compiler_params=params(),
        name="hot",
    )(hot_grad, hot_table, hot_accum.reshape(1, hot_rows))
    return (
        new_hot_table,
        new_hot_accum.reshape(hot_rows),
        new_cold_table,
        new_cold_accum.reshape(shard),
    )


def solution(mesh):
    return jax.shard_map(
        on_device,
        mesh=mesh,
        in_specs=(
            P(ALL, None),
            P(ALL, None),
            P(ALL, None),
            P(),
            P(),
            P("rows", None),
            P("rows"),
            P(),
            P(),
            P(),
            P(),
            P(ALL, None),
        ),
        out_specs=(P(), P(), P("rows", None), P("rows")),
        check_vma=False,
    )
```

```python
import functools

import jax
import jax.numpy as jnp
from jax import lax
from jax.experimental import pallas as pl
from jax.experimental.pallas import tpu as pltpu
from jax.sharding import PartitionSpec as P

HEAD = 128
STEP_RATE = 0.5
LANES = 128
SUBLANES = 8
ALL = ("rows", "rep")
F32 = jnp.float32
BF16 = jnp.bfloat16

VMEM = pl.BlockSpec(memory_space=pltpu.VMEM)
ANY = pl.BlockSpec(memory_space=pl.ANY)


def params(mib=24):
    return pltpu.CompilerParams(vmem_limit_bytes=mib << 20)


def dot(a, b, dims, precision=None):
    return lax.dot_general(
        a, b, (dims, ((), ())), preferred_element_type=F32, precision=precision
    )


NN = ((1,), (0,))
NT = ((1,), (1,))
TN = ((0,), (0,))


def gather_kernel(asked_ref, table_ref, out_ref, rows_scr, *, n_rows, n_rep, slot):
    j = lax.axis_index("rows")
    p = lax.axis_index("rep")
    shard = table_ref.shape[0]
    width = table_ref.shape[1] // 3
    chunks = width // LANES

    for r in range(n_rows):
        rows_scr[r : r + 1, :] = asked_ref[r * n_rep + p]
    asked = rows_scr[...]
    pos = lax.broadcasted_iota(jnp.int32, asked.shape, 1)
    picks = []
    for k in range(slot):
        col = jnp.sum(jnp.where(pos == j * slot + k, asked, 0), axis=1, keepdims=True)
        picks.append((lax.broadcasted_iota(jnp.int32, (n_rows, shard), 1) == col).astype(F32))
    pick = jnp.concatenate(picks, axis=0).astype(BF16)
    rows = dot(pick, table_ref[...], NN)
    rows = rows[:, 0:width] + rows[:, width : 2 * width] + rows[:, 2 * width : 3 * width]
    for k in range(slot):
        for c in range(chunks):
            out_ref[:, k * chunks + c, :] = rows[
                k * n_rows : (k + 1) * n_rows, c * LANES : (c + 1) * LANES
            ]


def normalise(x, eps):
    cent = x - jnp.mean(x, axis=1, keepdims=True)
    rstd = lax.rsqrt(jnp.mean(cent * cent, axis=1, keepdims=True) + eps)
    return cent * rstd, rstd


def project(x_hat, gain, bias, w_in):
    pre = dot((x_hat * gain + bias).astype(BF16), w_in, NN)
    sig = jax.nn.sigmoid(pre)
    return (pre * sig).astype(BF16), sig * (1.0 + pre * (1.0 - sig))


def early_kernel(
    event_hbm,
    count_hbm,
    hot_hbm,
    gain_hbm,
    bias_hbm,
    w_in_hbm,
    w_out_hbm,
    grad_hbm,
    cold_hbm,
    w_in_ref,
    proj_ref,
    pick_ref,
    live_ref,
    gain_ref,
    bias_ref,
    parts_ref,
    gated_out,
    scatter_out,
    dsilu_out,
    hat_out,
    rstd_out,
    base_out,
    gated_ref,
    scatter_ref,
    dsilu_ref,
    hat_ref,
    rstd_ref,
    base_ref,
    event_scr,
    count_scr,
    hot_scr,
    w_out_scr,
    grad_scr,
    cold_scr,
    sems,
    out_sems,
    *,
    n_owner,
    slot,
):
    copies = [
        pltpu.make_async_copy(src, dst, sems.at[i])
        for i, (src, dst) in enumerate(
            (
                (cold_hbm, cold_scr),
                (event_hbm, event_scr),
                (count_hbm, count_scr),
                (hot_hbm, hot_scr),
                (gain_hbm, gain_ref),
                (bias_hbm, bias_ref),
                (grad_hbm, grad_scr),
                (w_out_hbm, w_out_scr),
                (w_in_hbm, w_in_ref),
            )
        )
    ]
    for copy in copies:
        copy.start()
    sends = {
        name: pltpu.make_async_copy(src, dst, out_sems.at[i])
        for i, (name, src, dst) in enumerate(
            (
                ("gated", gated_ref, gated_out),
                ("scatter", scatter_ref, scatter_out),
                ("dsilu", dsilu_ref, dsilu_out),
                ("hat", hat_ref, hat_out),
                ("rstd", rstd_ref, rstd_out),
                ("base", base_ref, base_out),
            )
        )
    }
    hot_rows, width = hot_scr.shape
    seq = grad_scr.shape[0]
    slots = scatter_ref.shape[0]
    fetched = slots - hot_rows

    copies[0].wait()
    cold = cold_scr[...]
    high = cold.astype(BF16)
    rest = cold - high.astype(F32)
    mid = rest.astype(BF16)
    parts_ref[:, 0:width] = high
    parts_ref[:, width : 2 * width] = mid
    parts_ref[:, 2 * width : 3 * width] = (rest - mid.astype(F32)).astype(BF16)

    copies[1].wait()
    copies[2].wait()
    event_row = event_scr[...]
    scatter = (
        lax.broadcasted_iota(jnp.int32, (slots, seq), 0) == jnp.broadcast_to(event_row, (slots, seq))
    ).astype(F32)
    scatter_ref[...] = scatter.astype(BF16)
    sends["scatter"].start()
    pick_ref[...] = jnp.transpose(scatter[hot_rows:slots, :]).astype(BF16)
    owner = lax.broadcasted_iota(jnp.int32, (fetched, n_owner), 0) // slot
    mine = owner == lax.broadcasted_iota(jnp.int32, (fetched, n_owner), 1)
    counts = jnp.broadcast_to(count_scr[...], (fetched, n_owner))
    count_col = jnp.sum(jnp.where(mine, counts, 0), axis=1, keepdims=True)
    turn = lax.broadcasted_iota(jnp.int32, (fetched, LANES), 0) % slot
    live_ref[...] = (turn < count_col).astype(F32)

    for i in (3, 4, 5):
        copies[i].wait()
    x_hat, rstd = normalise(hot_scr[...], 1e-05)
    hat_ref[...] = x_hat
    rstd_ref[...] = jnp.broadcast_to(rstd, (hot_rows, LANES))
    sends["hat"].start()
    sends["rstd"].start()

    copies[6].wait()
    grad = grad_scr[...]
    base_ref[...] = dot(scatter.astype(BF16), grad, NN)
    sends["base"].start()
    copies[7].wait()
    gated_ref[...] = dot(grad, w_out_scr[...], NT).astype(BF16)
    sends["gated"].start()
    copies[8].wait()
    proj, dsilu = project(x_hat, gain_ref[...], bias_ref[...], w_in_ref[...])
    dsilu_ref[...] = dsilu
    sends["dsilu"].start()
    proj_ref[...] = dot(scatter[0:hot_rows, :].astype(BF16), proj, TN).astype(BF16)
    for send in sends.values():
        send.wait()


def layer_kernel(
    fetched_ref,
    w_in_ref,
    proj_ref,
    pick_ref,
    live_ref,
    gain_ref,
    bias_ref,
    gated_hbm,
    scatter_hbm,
    dsilu_hbm,
    hat_hbm,
    rstd_hbm,
    base_hbm,
    out_ref,
    x_scr,
    g_scr,
    gated_ref,
    scatter_ref,
    dsilu_ref,
    hat_ref,
    rstd_ref,
    base_ref,
    sems,
    *,
    n_dev,
    n_rep,
    slot,
):
    copies = [
        pltpu.make_async_copy(src, dst, sems.at[i])
        for i, (src, dst) in enumerate(
            (
                (gated_hbm, gated_ref),
                (scatter_hbm, scatter_ref),
                (dsilu_hbm, dsilu_ref),
                (hat_hbm, hat_ref),
                (rstd_hbm, rstd_ref),
                (base_hbm, base_ref),
            )
        )
    ]
    for copy in copies:
        copy.start()
    hot_rows, width = hat_ref.shape
    n_owner = fetched_ref.shape[0]
    chunks = width // LANES
    slots = scatter_ref.shape[0]
    seq, inner = gated_ref.shape
    heads = inner // HEAD
    gain = gain_ref[...]

    for j in range(n_owner):
        for k in range(slot):
            for c in range(chunks):
                x_scr[j * slot + k : j * slot + k + 1, c * LANES : (c + 1) * LANES] = fetched_ref[
                    j, k * chunks + c : k * chunks + c + 1, :
                ]
    live = live_ref[:, 0:1]
    cold_hat, cold_rstd = normalise(x_scr[...] * live, 1e-05)
    cold_proj, cold_dsilu = project(cold_hat, gain, bias_ref[...], w_in_ref[...])
    proj_ev = (proj_ref[...].astype(F32) + dot(pick_ref[...], cold_proj, NN)).astype(BF16)
    gates = proj_ev[:, 0:inner].astype(F32)

    scale = HEAD ** (-0.5)
    causal = (
        lax.broadcasted_iota(jnp.int32, (seq, seq), 0)
        >= lax.broadcasted_iota(jnp.int32, (seq, seq), 1)
    ).astype(F32) * (1.0 / seq)

    values, queries, keys, atts, dacts, mixeds = [], [], [], [], [], []
    for h in range(heads):
        lo = h * HEAD
        v = proj_ev[:, inner + lo : inner + lo + HEAD]
        q = proj_ev[:, 2 * inner + lo : 2 * inner + lo + HEAD]
        kk = proj_ev[:, 3 * inner + lo : 3 * inner + lo + HEAD]
        s = dot(q, kk, NT) * scale
        sg = jax.nn.sigmoid(s)
        a = (s * sg * causal).astype(BF16)
        dacts.append(sg * (1.0 + s * (1.0 - sg)) * causal)
        values.append(v)
        queries.append(q)
        keys.append(kk)
        atts.append(a)
        mixeds.append(dot(a, v, NN))
    y, mrstd = normalise(jnp.concatenate(mixeds, axis=1), 1e-06)

    copies[0].wait()
    d_gated = gated_ref[...].astype(F32)
    d_gates = (d_gated * y).astype(BF16)
    d_y = d_gated * gates
    d_mixed = mrstd * (
        d_y - jnp.mean(d_y, axis=1, keepdims=True) - y * jnp.mean(d_y * y, axis=1, keepdims=True)
    )
    d_mixed = d_mixed.astype(BF16)
    d_vs, d_qs, d_ks = [], [], []
    for h in range(heads):
        dm = d_mixed[:, h * HEAD : (h + 1) * HEAD]
        d_a = dot(dm, values[h], NT).astype(BF16).astype(F32)
        d_vs.append(dot(atts[h], dm, TN).astype(BF16))
        d_s = (d_a * dacts[h] * scale).astype(BF16)
        d_qs.append(dot(d_s, keys[h], NN).astype(BF16))
        d_ks.append(dot(d_s, queries[h], TN).astype(BF16))
    d_proj = jnp.concatenate([d_gates] + d_vs + d_qs + d_ks, axis=1)

    for copy in copies[1:]:
        copy.wait()
    d_slot = dot(scatter_ref[...], d_proj, NN)
    d_pre = jnp.concatenate(
        [d_slot[0:hot_rows] * dsilu_ref[...], d_slot[hot_rows:slots] * cold_dsilu], axis=0
    ).astype(BF16)
    d_hat = dot(d_pre, w_in_ref[...], NT) * gain

    def back(d, x_hat, rstd):
        return rstd * (
            d - jnp.mean(d, axis=1, keepdims=True) - x_hat * jnp.mean(d * x_hat, axis=1, keepdims=True)
        )

    hot = back(d_hat[0:hot_rows], hat_ref[...], rstd_ref[:, 0:1]) + base_ref[0:hot_rows, :]
    cold = back(d_hat[hot_rows:slots], cold_hat, cold_rstd) + base_ref[hot_rows:slots, :]
    x_scr[...] = cold * live

    units = hot_rows * chunks
    share = units // n_dev
    if share < SUBLANES:
        g_scr[...] = hot
    for g in range(hot_rows // SUBLANES):
        for c in range(chunks):
            first = (g * chunks + c) * SUBLANES
            at = (slice(g * SUBLANES, (g + 1) * SUBLANES), slice(c * LANES, (c + 1) * LANES))
            if share >= SUBLANES:
                out_ref[first // share, first % share : first % share + SUBLANES, :] = hot[at]
            else:
                for i in range(SUBLANES):
                    q = first + i
                    row = g * SUBLANES + i
                    out_ref[q // share, q % share : q % share + 1, :] = g_scr[row : row + 1, at[1]]

    for j in range(n_owner):
        for k in range(slot):
            for c in range(chunks):
                at = j * slot + k
                row = x_scr[at : at + 1, c * LANES : (c + 1) * LANES]
                to = share + k * chunks + c
                for p in range(n_rep):
                    out_ref[j * n_rep + p, to : to + 1, :] = row


def sum_kernel(got_ref, out_ref, *, share):
    n_dev = out_ref.shape[0]
    total = got_ref[0, 0:share, :]
    for d in range(1, n_dev):
        total = total + got_ref[d, 0:share, :]
    for d in range(n_dev):
        out_ref[d] = total


def cold_kernel(asked_ref, got_ref, table_ref, accum_ref, new_ref, new_accum_ref, *, slot, share):
    j = lax.axis_index("rows")
    n_dev = asked_ref.shape[0]
    shard, width = table_ref.shape
    chunks = width // LANES
    asked = asked_ref[:, 0, :]
    pos = lax.broadcasted_iota(jnp.int32, asked.shape, 1)
    picks = []
    for k in range(slot):
        col = jnp.sum(jnp.where(pos == j * slot + k, asked, 0), axis=1, keepdims=True)
        picks.append(
            (lax.broadcasted_iota(jnp.int32, (n_dev, shard), 1) == col).astype(F32)
        )
    grads = []
    for c in range(chunks):
        part = None
        for k in range(slot):
            rows = got_ref[:, share + k * chunks + c, :]
            one = dot(picks[k], rows, TN, lax.Precision.HIGHEST)
            part = one if part is None else part + one
        grads.append(part)
    total = grads[0] * grads[0]
    for g in grads[1:]:
        total = total + g * g
    mean_sq = jnp.sum(total, axis=1, keepdims=True) * (1.0 / width)
    wide = jnp.transpose(jnp.broadcast_to(mean_sq, (shard, LANES)))
    accum_row = accum_ref[...]
    new_accum_ref[...] = accum_row + wide[0:1, :]
    accum_col = jnp.transpose(jnp.broadcast_to(accum_row, (LANES, shard)))[:, 0:1]
    step = lax.rsqrt(accum_col + mean_sq) * STEP_RATE
    for c in range(chunks):
        cols = slice(c * LANES, (c + 1) * LANES)
        new_ref[:, cols] = table_ref[:, cols] - grads[c] * step


def hot_kernel(got_ref, table_ref, accum_ref, new_ref, new_accum_ref, g_scr):
    n_dev, share, _ = got_ref.shape
    rows, width = table_ref.shape
    chunks = width // LANES
    for g in range(rows // SUBLANES):
        for c in range(chunks):
            first = (g * chunks + c) * SUBLANES
            at = (slice(g * SUBLANES, (g + 1) * SUBLANES), slice(c * LANES, (c + 1) * LANES))
            if share >= SUBLANES:
                g_scr[at] = got_ref[first // share, first % share : first % share + SUBLANES, :]
            else:
                for i in range(SUBLANES):
                    q = first + i
                    g_scr[g * SUBLANES + i : g * SUBLANES + i + 1, at[1]] = got_ref[
                        q // share, q % share : q % share + 1, :
                    ]
    grad = g_scr[...]
    mean_sq = jnp.mean(grad * grad, axis=1, keepdims=True)
    wide = jnp.transpose(jnp.broadcast_to(mean_sq, (rows, LANES)))
    accum_row = accum_ref[...]
    new_accum_ref[...] = accum_row + wide[0:1, :]
    accum_col = jnp.transpose(jnp.broadcast_to(accum_row, (LANES, rows)))[:, 0:1]
    new_ref[...] = table_ref[...] - STEP_RATE * grad * lax.rsqrt(accum_col + mean_sq)


def on_device(
    event_slots,
    fetch_rows,
    fetch_counts,
    hot_table,
    hot_accum,
    cold_table,
    cold_accum,
    ln_gain,
    ln_bias,
    w_in,
    w_out,
    out_grad,
):
    n_rows = lax.axis_size("rows")
    n_rep = lax.axis_size("rep")
    n_dev = n_rows * n_rep
    slot = fetch_rows.shape[1] // n_rows
    hot_rows, width = hot_table.shape
    shard = cold_table.shape[0]
    chunks = width // LANES
    share = hot_rows * chunks // n_dev
    asks = fetch_rows.shape[1]
    slots = hot_rows + asks
    seq, inner = out_grad.shape[0], w_out.shape[0]

    with jax.named_scope("asks"):
        asked = lax.all_to_all(
            jnp.broadcast_to(fetch_rows.reshape(1, 1, asks), (n_dev, 1, asks)), ALL, 0, 0, tiled=True
        )
    late = (
        ((seq, inner), BF16),
        ((slots, seq), BF16),
        ((hot_rows, w_in.shape[1]), F32),
        ((hot_rows, width), F32),
        ((hot_rows, LANES), F32),
        ((slots, width), F32),
    )
    early = pl.pallas_call(
        functools.partial(early_kernel, n_owner=n_rows, slot=slot),
        out_shape=(
            pltpu.VMEM(w_in.shape, BF16),
            pltpu.VMEM((seq, w_in.shape[1]), BF16),
            pltpu.VMEM((seq, asks), BF16),
            pltpu.VMEM((asks, LANES), F32),
            pltpu.VMEM((1, width), F32),
            pltpu.VMEM((1, width), F32),
            pltpu.VMEM((shard, 3 * width), BF16),
        )
        + tuple(pltpu.HBM(*x) for x in late),
        in_specs=[ANY] * 9,
        out_specs=(VMEM,) * 7 + (ANY,) * 6,
        scratch_shapes=[pltpu.VMEM(*x) for x in late]
        + [
            pltpu.VMEM(event_slots.shape, jnp.int32),
            pltpu.VMEM(fetch_counts.shape, jnp.int32),
            pltpu.VMEM((hot_rows, width), F32),
            pltpu.VMEM(w_out.shape, BF16),
            pltpu.VMEM(out_grad.shape, BF16),
            pltpu.VMEM((shard, width), F32),
            pltpu.SemaphoreType.DMA((9,)),
            pltpu.SemaphoreType.DMA((6,)),
        ],
        compiler_params=params(),
        cost_estimate=pl.CostEstimate(flops=4 * 10**9, bytes_accessed=8 << 20, transcendentals=0),
        name="early",
    )(
        *(
            pltpu.with_memory_space_constraint(x, pltpu.HBM)
            for x in (
                event_slots,
                fetch_counts,
                hot_table,
                ln_gain.reshape(1, width),
                ln_bias.reshape(1, width),
                w_in,
                w_out,
                out_grad,
                cold_table,
            )
        )
    )
    early = [
        pltpu.with_memory_space_constraint(x, pltpu.VMEM if i < 7 else pltpu.HBM)
        for i, x in enumerate(early)
    ]
    found = pl.pallas_call(
        functools.partial(gather_kernel, n_rows=n_rows, n_rep=n_rep, slot=slot),
        out_shape=jax.ShapeDtypeStruct((n_rows, slot * chunks, LANES), F32),
        in_specs=[VMEM, VMEM],
        out_specs=VMEM,
        scratch_shapes=[pltpu.VMEM((n_rows, asks), jnp.int32)],
        compiler_params=params(),
        name="gather",
    )(asked, early[6])
    fetched = lax.all_to_all(found, "rows", 0, 0, tiled=True)

    sent = pl.pallas_call(
        functools.partial(layer_kernel, n_dev=n_dev, n_rep=n_rep, slot=slot),
        out_shape=jax.ShapeDtypeStruct((n_dev, share + slot * chunks, LANES), F32),
        in_specs=[VMEM] * 7 + [ANY] * 6,
        out_specs=VMEM,
        scratch_shapes=[pltpu.VMEM((asks, width), F32), pltpu.VMEM((hot_rows, width), F32)]
        + [pltpu.VMEM(*x) for x in late]
        + [pltpu.SemaphoreType.DMA((6,))],
        compiler_params=params(),
        name="layer",
    )(fetched, *early[:6], *early[7:])
    got = lax.all_to_all(sent, ALL, 0, 0, tiled=True)

    summed = pl.pallas_call(
        functools.partial(sum_kernel, share=share),
        out_shape=jax.ShapeDtypeStruct((n_dev, share, LANES), F32),
        in_specs=[VMEM],
        out_specs=VMEM,
        compiler_params=params(),
        name="sum",
    )(got)
    hot_grad = lax.all_to_all(summed, ALL, 0, 0, tiled=True)

    new_cold_table, new_cold_accum = pl.pallas_call(
        functools.partial(cold_kernel, slot=slot, share=share),
        out_shape=(
            jax.ShapeDtypeStruct((shard, width), F32),
            jax.ShapeDtypeStruct((1, shard), F32),
        ),
        in_specs=[VMEM] * 4,
        out_specs=(VMEM, VMEM),
        compiler_params=params(),
        name="cold",
    )(asked, got, cold_table, cold_accum.reshape(1, shard))

    new_hot_table, new_hot_accum = pl.pallas_call(
        hot_kernel,
        out_shape=(
            jax.ShapeDtypeStruct((hot_rows, width), F32),
            jax.ShapeDtypeStruct((1, hot_rows), F32),
        ),
        in_specs=[VMEM] * 3,
        out_specs=(VMEM, VMEM),
        scratch_shapes=[pltpu.VMEM((hot_rows, width), F32)],
        compiler_params=params(),
        name="hot",
    )(hot_grad, hot_table, hot_accum.reshape(1, hot_rows))
    return (
        new_hot_table,
        new_hot_accum.reshape(hot_rows),
        new_cold_table,
        new_cold_accum.reshape(shard),
    )


def solution(mesh):
    return jax.shard_map(
        on_device,
        mesh=mesh,
        in_specs=(
            P(ALL, None),
            P(ALL, None),
            P(ALL, None),
            P(),
            P(),
            P("rows", None),
            P("rows"),
            P(),
            P(),
            P(),
            P(),
            P(ALL, None),
        ),
        out_specs=(P(), P(), P("rows", None), P("rows")),
        check_vma=False,
    )
```

```python
import functools

import jax
import jax.numpy as jnp
from jax import lax
from jax.experimental import pallas as pl
from jax.experimental.pallas import tpu as pltpu
from jax.sharding import PartitionSpec as P

HEAD = 128
STEP_RATE = 0.5
LANES = 128
SUBLANES = 8
ALL = ("rows", "rep")
F32 = jnp.float32
BF16 = jnp.bfloat16

VMEM = pl.BlockSpec(memory_space=pltpu.VMEM)
ANY = pl.BlockSpec(memory_space=pl.ANY)


def params(mib=24):
    return pltpu.CompilerParams(vmem_limit_bytes=mib << 20)


def dot(a, b, dims, precision=None):
    return lax.dot_general(
        a, b, (dims, ((), ())), preferred_element_type=F32, precision=precision
    )


NN = ((1,), (0,))
NT = ((1,), (1,))
TN = ((0,), (0,))


def ask_kernel(rows_hbm, out_ref, rows_scr, sem):
    copy = pltpu.make_async_copy(rows_hbm, rows_scr, sem)
    copy.start()
    copy.wait()
    out_ref[...] = jnp.broadcast_to(rows_scr[...][None], out_ref.shape)


def even(n):
    return n + n % 2


def gather_kernel(asked_ref, table_ref, out_ref, rows_scr, *, n_rows, n_rep, slot):
    j = lax.axis_index("rows")
    p = lax.axis_index("rep")
    shard = table_ref.shape[0]
    width = table_ref.shape[1] // 3
    chunks = width // LANES

    for r in range(n_rows):
        rows_scr[r : r + 1, :] = asked_ref[r * n_rep + p]
    asked = rows_scr[...]
    pos = lax.broadcasted_iota(jnp.int32, asked.shape, 1)
    picks = []
    for k in range(slot):
        col = jnp.sum(jnp.where(pos == j * slot + k, asked, 0), axis=1, keepdims=True)
        picks.append((lax.broadcasted_iota(jnp.int32, (n_rows, shard), 1) == col).astype(F32))
    pick = jnp.concatenate(picks, axis=0).astype(BF16)
    rows = dot(pick, table_ref[...], NN)
    rows = rows[:, 0:width] + rows[:, width : 2 * width] + rows[:, 2 * width : 3 * width]
    for k in range(slot):
        for c in range(chunks):
            out_ref[:, k * chunks + c, :] = rows[
                k * n_rows : (k + 1) * n_rows, c * LANES : (c + 1) * LANES
            ]


def normalise(x, eps):
    cent = x - jnp.mean(x, axis=1, keepdims=True)
    rstd = lax.rsqrt(jnp.mean(cent * cent, axis=1, keepdims=True) + eps)
    return cent * rstd, rstd


def project(x_hat, gain, bias, w_in):
    pre = dot((x_hat * gain + bias).astype(BF16), w_in, NN)
    sig = jax.nn.sigmoid(pre)
    return (pre * sig).astype(BF16), sig * (1.0 + pre * (1.0 - sig))


def early_kernel(
    event_hbm,
    count_hbm,
    hot_hbm,
    gain_hbm,
    bias_hbm,
    w_in_hbm,
    w_out_hbm,
    grad_hbm,
    cold_hbm,
    w_in_ref,
    proj_ref,
    pick_ref,
    live_ref,
    gain_ref,
    bias_ref,
    parts_ref,
    gated_out,
    scatter_out,
    dsilu_out,
    hat_out,
    rstd_out,
    base_out,
    gated_ref,
    scatter_ref,
    dsilu_ref,
    hat_ref,
    rstd_ref,
    base_ref,
    event_scr,
    count_scr,
    hot_scr,
    w_out_scr,
    grad_scr,
    cold_scr,
    sems,
    out_sems,
    *,
    n_owner,
    slot,
):
    copies = [
        pltpu.make_async_copy(src, dst, sems.at[i])
        for i, (src, dst) in enumerate(
            (
                (cold_hbm, cold_scr),
                (event_hbm, event_scr),
                (count_hbm, count_scr),
                (hot_hbm, hot_scr),
                (gain_hbm, gain_ref),
                (bias_hbm, bias_ref),
                (grad_hbm, grad_scr),
                (w_out_hbm, w_out_scr),
                (w_in_hbm, w_in_ref),
            )
        )
    ]
    for copy in copies:
        copy.start()
    sends = {
        name: pltpu.make_async_copy(src, dst, out_sems.at[i])
        for i, (name, src, dst) in enumerate(
            (
                ("gated", gated_ref, gated_out),
                ("scatter", scatter_ref, scatter_out),
                ("dsilu", dsilu_ref, dsilu_out),
                ("hat", hat_ref, hat_out),
                ("rstd", rstd_ref, rstd_out),
                ("base", base_ref, base_out),
            )
        )
    }
    hot_rows, width = hot_scr.shape
    seq = grad_scr.shape[0]
    slots = scatter_ref.shape[0]
    fetched = slots - hot_rows

    copies[0].wait()
    cold = cold_scr[...]
    high = cold.astype(BF16)
    rest = cold - high.astype(F32)
    mid = rest.astype(BF16)
    parts_ref[:, 0:width] = high
    parts_ref[:, width : 2 * width] = mid
    parts_ref[:, 2 * width : 3 * width] = (rest - mid.astype(F32)).astype(BF16)

    copies[1].wait()
    copies[2].wait()
    event_row = event_scr[...]
    scatter = (
        lax.broadcasted_iota(jnp.int32, (slots, seq), 0) == jnp.broadcast_to(event_row, (slots, seq))
    ).astype(F32)
    scatter_ref[...] = scatter.astype(BF16)
    sends["scatter"].start()
    pick_ref[...] = jnp.transpose(scatter[hot_rows:slots, :]).astype(BF16)
    owner = lax.broadcasted_iota(jnp.int32, (fetched, n_owner), 0) // slot
    mine = owner == lax.broadcasted_iota(jnp.int32, (fetched, n_owner), 1)
    counts = jnp.broadcast_to(count_scr[...], (fetched, n_owner))
    count_col = jnp.sum(jnp.where(mine, counts, 0), axis=1, keepdims=True)
    turn = lax.broadcasted_iota(jnp.int32, (fetched, LANES), 0) % slot
    live_ref[...] = (turn < count_col).astype(F32)

    for i in (3, 4, 5):
        copies[i].wait()
    x_hat, rstd = normalise(hot_scr[...], 1e-05)
    hat_ref[...] = x_hat
    rstd_ref[...] = jnp.broadcast_to(rstd, (hot_rows, LANES))
    sends["hat"].start()
    sends["rstd"].start()

    copies[6].wait()
    grad = grad_scr[...]
    base_ref[...] = dot(scatter.astype(BF16), grad, NN)
    sends["base"].start()
    copies[7].wait()
    gated_ref[...] = dot(grad, w_out_scr[...], NT).astype(BF16)
    sends["gated"].start()
    copies[8].wait()
    proj, dsilu = project(x_hat, gain_ref[...], bias_ref[...], w_in_ref[...])
    dsilu_ref[...] = dsilu
    sends["dsilu"].start()
    proj_ref[...] = dot(scatter[0:hot_rows, :].astype(BF16), proj, TN).astype(BF16)
    for send in sends.values():
        send.wait()


def layer_kernel(
    fetched_ref,
    w_in_ref,
    proj_ref,
    pick_ref,
    live_ref,
    gain_ref,
    bias_ref,
    gated_hbm,
    scatter_hbm,
    dsilu_hbm,
    hat_hbm,
    rstd_hbm,
    base_hbm,
    out_ref,
    x_scr,
    g_scr,
    gated_ref,
    scatter_ref,
    dsilu_ref,
    hat_ref,
    rstd_ref,
    base_ref,
    sems,
    *,
    n_dev,
    n_rep,
    slot,
):
    copies = [
        pltpu.make_async_copy(src, dst, sems.at[i])
        for i, (src, dst) in enumerate(
            (
                (gated_hbm, gated_ref),
                (scatter_hbm, scatter_ref),
                (dsilu_hbm, dsilu_ref),
                (hat_hbm, hat_ref),
                (rstd_hbm, rstd_ref),
                (base_hbm, base_ref),
            )
        )
    ]
    for copy in copies:
        copy.start()
    hot_rows, width = hat_ref.shape
    n_owner = fetched_ref.shape[0]
    chunks = width // LANES
    slots = scatter_ref.shape[0]
    seq, inner = gated_ref.shape
    heads = inner // HEAD
    gain = gain_ref[...]

    for j in range(n_owner):
        for k in range(slot):
            for c in range(chunks):
                x_scr[j * slot + k : j * slot + k + 1, c * LANES : (c + 1) * LANES] = fetched_ref[
                    j, k * chunks + c : k * chunks + c + 1, :
                ]
    live = live_ref[:, 0:1]
    cold_hat, cold_rstd = normalise(x_scr[...] * live, 1e-05)
    cold_proj, cold_dsilu = project(cold_hat, gain, bias_ref[...], w_in_ref[...])
    proj_ev = (proj_ref[...].astype(F32) + dot(pick_ref[...], cold_proj, NN)).astype(BF16)
    gates = proj_ev[:, 0:inner].astype(F32)

    scale = HEAD ** (-0.5)
    causal = (
        lax.broadcasted_iota(jnp.int32, (seq, seq), 0)
        >= lax.broadcasted_iota(jnp.int32, (seq, seq), 1)
    ).astype(F32) * (1.0 / seq)

    values, queries, keys, atts, dacts, mixeds = [], [], [], [], [], []
    for h in range(heads):
        lo = h * HEAD
        v = proj_ev[:, inner + lo : inner + lo + HEAD]
        q = proj_ev[:, 2 * inner + lo : 2 * inner + lo + HEAD]
        kk = proj_ev[:, 3 * inner + lo : 3 * inner + lo + HEAD]
        s = dot(q, kk, NT) * scale
        sg = jax.nn.sigmoid(s)
        a = (s * sg * causal).astype(BF16)
        dacts.append(sg * (1.0 + s * (1.0 - sg)) * causal)
        values.append(v)
        queries.append(q)
        keys.append(kk)
        atts.append(a)
        mixeds.append(dot(a, v, NN))
    y, mrstd = normalise(jnp.concatenate(mixeds, axis=1), 1e-06)

    copies[0].wait()
    d_gated = gated_ref[...].astype(F32)
    d_gates = (d_gated * y).astype(BF16)
    d_y = d_gated * gates
    d_mixed = mrstd * (
        d_y - jnp.mean(d_y, axis=1, keepdims=True) - y * jnp.mean(d_y * y, axis=1, keepdims=True)
    )
    d_mixed = d_mixed.astype(BF16)
    d_vs, d_qs, d_ks = [], [], []
    for h in range(heads):
        dm = d_mixed[:, h * HEAD : (h + 1) * HEAD]
        d_a = dot(dm, values[h], NT).astype(BF16).astype(F32)
        d_vs.append(dot(atts[h], dm, TN).astype(BF16))
        d_s = (d_a * dacts[h] * scale).astype(BF16)
        d_qs.append(dot(d_s, keys[h], NN).astype(BF16))
        d_ks.append(dot(d_s, queries[h], TN).astype(BF16))
    d_proj = jnp.concatenate([d_gates] + d_vs + d_qs + d_ks, axis=1)

    for copy in copies[1:]:
        copy.wait()
    d_slot = dot(scatter_ref[...], d_proj, NN)
    d_pre = jnp.concatenate(
        [d_slot[0:hot_rows] * dsilu_ref[...], d_slot[hot_rows:slots] * cold_dsilu], axis=0
    ).astype(BF16)
    d_hat = dot(d_pre, w_in_ref[...], NT) * gain

    def back(d, x_hat, rstd):
        return rstd * (
            d - jnp.mean(d, axis=1, keepdims=True) - x_hat * jnp.mean(d * x_hat, axis=1, keepdims=True)
        )

    hot = back(d_hat[0:hot_rows], hat_ref[...], rstd_ref[:, 0:1]) + base_ref[0:hot_rows, :]
    cold = back(d_hat[hot_rows:slots], cold_hat, cold_rstd) + base_ref[hot_rows:slots, :]
    x_scr[...] = cold * live

    share = hot_rows * chunks // n_dev
    if share % SUBLANES:
        g_scr[...] = hot
    for g in range(hot_rows // SUBLANES):
        for c in range(chunks):
            first = (g * chunks + c) * SUBLANES
            at = (slice(g * SUBLANES, (g + 1) * SUBLANES), slice(c * LANES, (c + 1) * LANES))
            if share % SUBLANES == 0:
                off = first % share // 2
                out_ref[first // share, off : off + SUBLANES // 2] = hot[at].reshape(
                    SUBLANES // 2, 2, LANES
                )
            else:
                for i in range(SUBLANES):
                    to, off = divmod(first + i, share)
                    row = g * SUBLANES + i
                    out_ref[to, off // 2, off % 2 : off % 2 + 1, :] = g_scr[row : row + 1, at[1]]

    part = chunks // n_rep
    base = even(share) // 2
    for j in range(n_owner):
        for c in range(chunks):
            to = j * n_rep + c // part
            cols = slice(c * LANES, (c + 1) * LANES)
            if part == 1 and slot == 2:
                out_ref[to, base] = x_scr[j * slot : (j + 1) * slot, cols]
            else:
                for k in range(slot):
                    off = k * part + c % part
                    at = j * slot + k
                    out_ref[to, base + off // 2, off % 2 : off % 2 + 1, :] = x_scr[at : at + 1, cols]


def sum_kernel(got_ref, out_ref, cold_ref):
    n_dev, share, _ = out_ref.shape
    base = even(share) // 2
    total = got_ref[0, 0:base]
    for d in range(1, n_dev):
        total = total + got_ref[d, 0:base]
    total = total.reshape(2 * base, LANES)[0:share]
    for d in range(n_dev):
        out_ref[d] = total
    cold_ref[...] = got_ref[:, base:]


def cold_kernel(asked_ref, *refs, slot, n_rep):
    part_refs = refs[:n_rep]
    table_ref, accum_ref, new_ref, new_accum_ref, part_scr = refs[n_rep:]
    j = lax.axis_index("rows")
    p = lax.axis_index("rep")
    n_dev = asked_ref.shape[0]
    shard, width = table_ref.shape
    chunks = width // LANES
    part = chunks // n_rep
    for s in range(n_rep):
        part_scr[(p + n_rep - s) % n_rep] = part_refs[s][...]
    asked = asked_ref[:, 0, :]
    pos = lax.broadcasted_iota(jnp.int32, asked.shape, 1)
    picks = []
    for k in range(slot):
        col = jnp.sum(jnp.where(pos == j * slot + k, asked, 0), axis=1, keepdims=True)
        picks.append((lax.broadcasted_iota(jnp.int32, (n_dev, shard), 1) == col).astype(F32))
    pick = jnp.concatenate(picks, axis=0)
    grads = []
    for c in range(chunks):
        rows = []
        for k in range(slot):
            off = k * part + c % part
            rows.append(part_scr[c // part, :, off // 2, off % 2, :])
        grads.append(dot(pick, jnp.concatenate(rows, axis=0), TN, lax.Precision.HIGHEST))
    total = grads[0] * grads[0]
    for g in grads[1:]:
        total = total + g * g
    mean_sq = jnp.sum(total, axis=1, keepdims=True) * (1.0 / width)
    wide = jnp.transpose(jnp.broadcast_to(mean_sq, (shard, LANES)))
    accum_row = accum_ref[...]
    new_accum_ref[...] = accum_row + wide[0:1, :]
    accum_col = jnp.transpose(jnp.broadcast_to(accum_row, (LANES, shard)))[:, 0:1]
    step = lax.rsqrt(accum_col + mean_sq) * STEP_RATE
    for c in range(chunks):
        cols = slice(c * LANES, (c + 1) * LANES)
        new_ref[:, cols] = table_ref[:, cols] - grads[c] * step


def hot_kernel(got_ref, table_ref, accum_ref, new_ref, new_accum_ref, g_scr):
    n_dev, share, _ = got_ref.shape
    rows, width = table_ref.shape
    chunks = width // LANES
    for g in range(rows // SUBLANES):
        for c in range(chunks):
            first = (g * chunks + c) * SUBLANES
            at = (slice(g * SUBLANES, (g + 1) * SUBLANES), slice(c * LANES, (c + 1) * LANES))
            if share >= SUBLANES:
                g_scr[at] = got_ref[first // share, first % share : first % share + SUBLANES, :]
            else:
                for i in range(SUBLANES):
                    q = first + i
                    g_scr[g * SUBLANES + i : g * SUBLANES + i + 1, at[1]] = got_ref[
                        q // share, q % share : q % share + 1, :
                    ]
    grad = g_scr[...]
    mean_sq = jnp.mean(grad * grad, axis=1, keepdims=True)
    wide = jnp.transpose(jnp.broadcast_to(mean_sq, (rows, LANES)))
    accum_row = accum_ref[...]
    new_accum_ref[...] = accum_row + wide[0:1, :]
    accum_col = jnp.transpose(jnp.broadcast_to(accum_row, (LANES, rows)))[:, 0:1]
    new_ref[...] = table_ref[...] - STEP_RATE * grad * lax.rsqrt(accum_col + mean_sq)


def on_device(
    event_slots,
    fetch_rows,
    fetch_counts,
    hot_table,
    hot_accum,
    cold_table,
    cold_accum,
    ln_gain,
    ln_bias,
    w_in,
    w_out,
    out_grad,
):
    n_rows = lax.axis_size("rows")
    n_rep = lax.axis_size("rep")
    n_dev = n_rows * n_rep
    slot = fetch_rows.shape[1] // n_rows
    hot_rows, width = hot_table.shape
    shard = cold_table.shape[0]
    chunks = width // LANES
    share = hot_rows * chunks // n_dev
    cold_pairs = even(slot * (chunks // n_rep)) // 2
    asks = fetch_rows.shape[1]
    slots = hot_rows + asks
    seq, inner = out_grad.shape[0], w_out.shape[0]

    with jax.named_scope("asks"):
        mine = pl.pallas_call(
            ask_kernel,
            out_shape=pltpu.VMEM((n_dev, 1, asks), jnp.int32),
            in_specs=[ANY],
            out_specs=VMEM,
            scratch_shapes=[pltpu.VMEM((1, asks), jnp.int32), pltpu.SemaphoreType.DMA],
            compiler_params=params(),
            name="ask",
        )(pltpu.with_memory_space_constraint(fetch_rows, pltpu.HBM))
        asked = lax.all_to_all(mine, ALL, 0, 0, tiled=True)
    late = (
        ((seq, inner), BF16),
        ((slots, seq), BF16),
        ((hot_rows, w_in.shape[1]), F32),
        ((hot_rows, width), F32),
        ((hot_rows, LANES), F32),
        ((slots, width), F32),
    )
    early = pl.pallas_call(
        functools.partial(early_kernel, n_owner=n_rows, slot=slot),
        out_shape=(
            pltpu.VMEM(w_in.shape, BF16),
            pltpu.VMEM((seq, w_in.shape[1]), BF16),
            pltpu.VMEM((seq, asks), BF16),
            pltpu.VMEM((asks, LANES), F32),
            pltpu.VMEM((1, width), F32),
            pltpu.VMEM((1, width), F32),
            pltpu.VMEM((shard, 3 * width), BF16),
        )
        + tuple(pltpu.HBM(*x) for x in late),
        in_specs=[ANY] * 9,
        out_specs=(VMEM,) * 7 + (ANY,) * 6,
        scratch_shapes=[pltpu.VMEM(*x) for x in late]
        + [
            pltpu.VMEM(event_slots.shape, jnp.int32),
            pltpu.VMEM(fetch_counts.shape, jnp.int32),
            pltpu.VMEM((hot_rows, width), F32),
            pltpu.VMEM(w_out.shape, BF16),
            pltpu.VMEM(out_grad.shape, BF16),
            pltpu.VMEM((shard, width), F32),
            pltpu.SemaphoreType.DMA((9,)),
            pltpu.SemaphoreType.DMA((6,)),
        ],
        compiler_params=params(),
        cost_estimate=pl.CostEstimate(flops=4 * 10**9, bytes_accessed=8 << 20, transcendentals=0),
        name="early",
    )(
        *(
            pltpu.with_memory_space_constraint(x, pltpu.HBM)
            for x in (
                event_slots,
                fetch_counts,
                hot_table,
                ln_gain.reshape(1, width),
                ln_bias.reshape(1, width),
                w_in,
                w_out,
                out_grad,
                cold_table,
            )
        )
    )
    early = [
        pltpu.with_memory_space_constraint(x, pltpu.VMEM if i < 7 else pltpu.HBM)
        for i, x in enumerate(early)
    ]
    found = pl.pallas_call(
        functools.partial(gather_kernel, n_rows=n_rows, n_rep=n_rep, slot=slot),
        out_shape=jax.ShapeDtypeStruct((n_rows, slot * chunks, LANES), F32),
        in_specs=[VMEM, VMEM],
        out_specs=VMEM,
        scratch_shapes=[pltpu.VMEM((n_rows, asks), jnp.int32)],
        compiler_params=params(),
        name="gather",
    )(asked, early[6])
    fetched = lax.all_to_all(found, "rows", 0, 0, tiled=True)

    sent = pl.pallas_call(
        functools.partial(layer_kernel, n_dev=n_dev, n_rep=n_rep, slot=slot),
        out_shape=jax.ShapeDtypeStruct((n_dev, even(share) // 2 + cold_pairs, 2, LANES), F32),
        in_specs=[VMEM] * 7 + [ANY] * 6,
        out_specs=VMEM,
        scratch_shapes=[pltpu.VMEM((asks, width), F32), pltpu.VMEM((hot_rows, width), F32)]
        + [pltpu.VMEM(*x) for x in late]
        + [pltpu.SemaphoreType.DMA((6,))],
        compiler_params=params(),
        name="layer",
    )(fetched, *early[:6], *early[7:])
    got = lax.all_to_all(sent, ALL, 0, 0, tiled=True)

    summed, cold_part = pl.pallas_call(
        sum_kernel,
        out_shape=(
            pltpu.VMEM((n_dev, share, LANES), F32),
            pltpu.VMEM((n_dev, cold_pairs, 2, LANES), F32),
        ),
        in_specs=[VMEM],
        out_specs=(VMEM, VMEM),
        compiler_params=params(),
        name="sum",
    )(got)
    hot_grad = lax.all_to_all(summed, ALL, 0, 0, tiled=True)
    parts = [cold_part] + [
        lax.ppermute(cold_part, "rep", [(i, (i + s) % n_rep) for i in range(n_rep)])
        for s in range(1, n_rep)
    ]

    new_cold_table, new_cold_accum = pl.pallas_call(
        functools.partial(cold_kernel, slot=slot, n_rep=n_rep),
        out_shape=(
            jax.ShapeDtypeStruct((shard, width), F32),
            jax.ShapeDtypeStruct((1, shard), F32),
        ),
        in_specs=[VMEM] * (n_rep + 3),
        out_specs=(VMEM, VMEM),
        scratch_shapes=[pltpu.VMEM((n_rep, n_dev, cold_pairs, 2, LANES), F32)],
        compiler_params=params(),
        name="cold",
    )(asked, *parts, cold_table, cold_accum.reshape(1, shard))

    new_hot_table, new_hot_accum = pl.pallas_call(
        hot_kernel,
        out_shape=(
            jax.ShapeDtypeStruct((hot_rows, width), F32),
            jax.ShapeDtypeStruct((1, hot_rows), F32),
        ),
        in_specs=[VMEM] * 3,
        out_specs=(VMEM, VMEM),
        scratch_shapes=[pltpu.VMEM((hot_rows, width), F32)],
        compiler_params=params(),
        name="hot",
    )(hot_grad, hot_table, hot_accum.reshape(1, hot_rows))
    return (
        new_hot_table,
        new_hot_accum.reshape(hot_rows),
        new_cold_table,
        new_cold_accum.reshape(shard),
    )


def solution(mesh):
    return jax.shard_map(
        on_device,
        mesh=mesh,
        in_specs=(
            P(ALL, None),
            P(ALL, None),
            P(ALL, None),
            P(),
            P(),
            P("rows", None),
            P("rows"),
            P(),
            P(),
            P(),
            P(),
            P(ALL, None),
        ),
        out_specs=(P(), P(), P("rows", None), P("rows")),
        check_vma=False,
    )
```

```python
import functools

import jax
import jax.numpy as jnp
from jax import lax
from jax.experimental import pallas as pl
from jax.experimental.pallas import tpu as pltpu
from jax.sharding import PartitionSpec as P

HEAD = 128
STEP_RATE = 0.5
LANES = 128
SUBLANES = 8
ALL = ("rows", "rep")
F32 = jnp.float32
BF16 = jnp.bfloat16

LONG = pl.CostEstimate(flops=10**10, bytes_accessed=16 << 20, transcendentals=0)

VMEM = pl.BlockSpec(memory_space=pltpu.VMEM)
ANY = pl.BlockSpec(memory_space=pl.ANY)


def params(mib=24):
    return pltpu.CompilerParams(vmem_limit_bytes=mib << 20)


def dot(a, b, dims, precision=None):
    return lax.dot_general(
        a, b, (dims, ((), ())), preferred_element_type=F32, precision=precision
    )


NN = ((1,), (0,))
NT = ((1,), (1,))
TN = ((0,), (0,))


def ask_kernel(rows_hbm, out_ref, rows_scr, sem):
    copy = pltpu.make_async_copy(rows_hbm, rows_scr, sem)
    copy.start()
    copy.wait()
    out_ref[...] = jnp.broadcast_to(rows_scr[...][None], out_ref.shape)


def even(n):
    return n + n % 2


def gather_kernel(asked_ref, table_ref, out_ref, rows_scr, *, n_rows, n_rep, slot):
    j = lax.axis_index("rows")
    p = lax.axis_index("rep")
    shard = table_ref.shape[0]
    width = table_ref.shape[1]
    chunks = width // LANES

    for r in range(n_rows):
        rows_scr[r : r + 1, :] = asked_ref[r * n_rep + p]
    asked = rows_scr[...]
    pos = lax.broadcasted_iota(jnp.int32, asked.shape, 1)
    picks = []
    for k in range(slot):
        col = jnp.sum(jnp.where(pos == j * slot + k, asked, 0), axis=1, keepdims=True)
        picks.append((lax.broadcasted_iota(jnp.int32, (n_rows, shard), 1) == col).astype(F32))
    pick = jnp.concatenate(picks, axis=0).astype(BF16)
    table = table_ref[...]
    high = table.astype(BF16)
    rest = table - high.astype(F32)
    mid = rest.astype(BF16)
    low = (rest - mid.astype(F32)).astype(BF16)
    rows = dot(pick, high, NN) + dot(pick, mid, NN) + dot(pick, low, NN)
    for k in range(slot):
        for c in range(chunks):
            out_ref[:, k * chunks + c, :] = rows[
                k * n_rows : (k + 1) * n_rows, c * LANES : (c + 1) * LANES
            ]


def normalise(x, eps):
    cent = x - jnp.mean(x, axis=1, keepdims=True)
    rstd = lax.rsqrt(jnp.mean(cent * cent, axis=1, keepdims=True) + eps)
    return cent * rstd, rstd


def project(x_hat, gain, bias, w_in):
    pre = dot((x_hat * gain + bias).astype(BF16), w_in, NN)
    sig = jax.nn.sigmoid(pre)
    return (pre * sig).astype(BF16), sig * (1.0 + pre * (1.0 - sig))


def layer_kernel(
    event_ref,
    count_ref,
    hot_ref,
    fetched_ref,
    gain_ref,
    bias_ref,
    w_in_ref,
    w_out_ref,
    grad_ref,
    out_ref,
    x_scr,
    g_scr,
    c_scr,
    *,
    n_dev,
    n_rep,
    slot,
):
    hot_rows, width = hot_ref.shape
    n_owner = fetched_ref.shape[0]
    chunks = width // LANES
    slots = x_scr.shape[0]
    fetched = slots - hot_rows
    seq = grad_ref.shape[0]
    inner = w_out_ref.shape[0]
    heads = inner // HEAD
    gain = gain_ref[...]

    owner = lax.broadcasted_iota(jnp.int32, (fetched, n_owner), 0) // slot
    mine = owner == lax.broadcasted_iota(jnp.int32, (fetched, n_owner), 1)
    counts = jnp.broadcast_to(count_ref[...], (fetched, n_owner))
    count_col = jnp.sum(jnp.where(mine, counts, 0), axis=1, keepdims=True)
    live = (lax.broadcasted_iota(jnp.int32, (fetched, 1), 0) % slot < count_col).astype(F32)

    for j in range(n_owner):
        for k in range(slot):
            at = j * slot + k
            for c in range(chunks):
                c_scr[at : at + 1, c * LANES : (c + 1) * LANES] = fetched_ref[
                    j, k * chunks + c : k * chunks + c + 1, :
                ]
    x_scr[0:hot_rows, :] = hot_ref[...]
    x_scr[hot_rows:slots, :] = c_scr[...] * live
    x_hat, rstd = normalise(x_scr[...], 1e-05)
    proj, dsilu = project(x_hat, gain, bias_ref[...], w_in_ref[...])

    scatter = (
        lax.broadcasted_iota(jnp.int32, (slots, seq), 0)
        == jnp.broadcast_to(event_ref[...], (slots, seq))
    ).astype(F32)
    scatter_b = scatter.astype(BF16)
    proj_ev = dot(scatter_b, proj, TN).astype(BF16)
    gates = proj_ev[:, 0:inner].astype(F32)

    scale = HEAD ** (-0.5)
    causal = (
        lax.broadcasted_iota(jnp.int32, (seq, seq), 0)
        >= lax.broadcasted_iota(jnp.int32, (seq, seq), 1)
    ).astype(F32) * (1.0 / seq)

    values, queries, keys, atts, dacts, mixeds = [], [], [], [], [], []
    for h in range(heads):
        lo = h * HEAD
        v = proj_ev[:, inner + lo : inner + lo + HEAD]
        q = proj_ev[:, 2 * inner + lo : 2 * inner + lo + HEAD]
        kk = proj_ev[:, 3 * inner + lo : 3 * inner + lo + HEAD]
        s = dot(q, kk, NT) * scale
        sg = jax.nn.sigmoid(s)
        a = (s * sg * causal).astype(BF16)
        dacts.append(sg * (1.0 + s * (1.0 - sg)) * causal)
        values.append(v)
        queries.append(q)
        keys.append(kk)
        atts.append(a)
        mixeds.append(dot(a, v, NN))
    y, mrstd = normalise(jnp.concatenate(mixeds, axis=1), 1e-06)

    grad = grad_ref[...]
    d_gated = dot(grad, w_out_ref[...], NT).astype(BF16).astype(F32)
    d_gates = (d_gated * y).astype(BF16)
    d_y = d_gated * gates
    d_mixed = mrstd * (
        d_y - jnp.mean(d_y, axis=1, keepdims=True) - y * jnp.mean(d_y * y, axis=1, keepdims=True)
    )
    d_mixed = d_mixed.astype(BF16)
    d_vs, d_qs, d_ks = [], [], []
    for h in range(heads):
        dm = d_mixed[:, h * HEAD : (h + 1) * HEAD]
        d_a = dot(dm, values[h], NT).astype(BF16).astype(F32)
        d_vs.append(dot(atts[h], dm, TN).astype(BF16))
        d_s = (d_a * dacts[h] * scale).astype(BF16)
        d_qs.append(dot(d_s, keys[h], NN).astype(BF16))
        d_ks.append(dot(d_s, queries[h], TN).astype(BF16))
    d_proj = jnp.concatenate([d_gates] + d_vs + d_qs + d_ks, axis=1)

    d_slot = dot(scatter_b, d_proj, NN)
    d_hat = dot((d_slot * dsilu).astype(BF16), w_in_ref[...], NT) * gain
    d_x = rstd * (
        d_hat
        - jnp.mean(d_hat, axis=1, keepdims=True)
        - x_hat * jnp.mean(d_hat * x_hat, axis=1, keepdims=True)
    )
    d_x = d_x + dot(scatter_b, grad, NN)
    hot = d_x[0:hot_rows]
    c_scr[...] = d_x[hot_rows:slots] * live

    share = hot_rows * chunks // n_dev
    if share % SUBLANES:
        g_scr[...] = hot
    for g in range(hot_rows // SUBLANES):
        for c in range(chunks):
            first = (g * chunks + c) * SUBLANES
            at = (slice(g * SUBLANES, (g + 1) * SUBLANES), slice(c * LANES, (c + 1) * LANES))
            if share % SUBLANES == 0:
                off = first % share // 2
                out_ref[first // share, off : off + SUBLANES // 2] = hot[at].reshape(
                    SUBLANES // 2, 2, LANES
                )
            else:
                for i in range(SUBLANES):
                    to, off = divmod(first + i, share)
                    row = g * SUBLANES + i
                    out_ref[to, off // 2, off % 2 : off % 2 + 1, :] = g_scr[row : row + 1, at[1]]

    part = chunks // n_rep
    base = even(share) // 2
    for j in range(n_owner):
        for c in range(chunks):
            to = j * n_rep + c // part
            cols = slice(c * LANES, (c + 1) * LANES)
            if part == 1 and slot == 2:
                out_ref[to, base] = c_scr[j * slot : (j + 1) * slot, cols]
            else:
                for k in range(slot):
                    off = k * part + c % part
                    at = j * slot + k
                    out_ref[to, base + off // 2, off % 2 : off % 2 + 1, :] = c_scr[at : at + 1, cols]


def sum_kernel(got_ref, out_ref, cold_ref):
    n_dev, share, _ = out_ref.shape
    base = even(share) // 2
    total = got_ref[0, 0:base]
    for d in range(1, n_dev):
        total = total + got_ref[d, 0:base]
    total = total.reshape(2 * base, LANES)[0:share]
    for d in range(n_dev):
        out_ref[d] = total
    cold_ref[...] = got_ref[:, base:]


def cold_kernel(asked_ref, *refs, slot, n_rep):
    part_refs = refs[:n_rep]
    table_ref, accum_ref, new_ref, new_accum_ref, part_scr = refs[n_rep:]
    j = lax.axis_index("rows")
    p = lax.axis_index("rep")
    n_dev = asked_ref.shape[0]
    shard, width = table_ref.shape
    chunks = width // LANES
    part = chunks // n_rep
    for s in range(n_rep):
        part_scr[(p + n_rep - s) % n_rep] = part_refs[s][...]
    asked = asked_ref[:, 0, :]
    pos = lax.broadcasted_iota(jnp.int32, asked.shape, 1)
    picks = []
    for k in range(slot):
        col = jnp.sum(jnp.where(pos == j * slot + k, asked, 0), axis=1, keepdims=True)
        picks.append((lax.broadcasted_iota(jnp.int32, (n_dev, shard), 1) == col).astype(F32))
    pick = jnp.concatenate(picks, axis=0)
    grads = []
    for c in range(chunks):
        rows = []
        for k in range(slot):
            off = k * part + c % part
            rows.append(part_scr[c // part, :, off // 2, off % 2, :])
        grads.append(dot(pick, jnp.concatenate(rows, axis=0), TN, lax.Precision.HIGHEST))
    total = grads[0] * grads[0]
    for g in grads[1:]:
        total = total + g * g
    mean_sq = jnp.sum(total, axis=1, keepdims=True) * (1.0 / width)
    wide = jnp.transpose(jnp.broadcast_to(mean_sq, (shard, LANES)))
    accum_row = accum_ref[...]
    new_accum_ref[...] = accum_row + wide[0:1, :]
    accum_col = jnp.transpose(jnp.broadcast_to(accum_row, (LANES, shard)))[:, 0:1]
    step = lax.rsqrt(accum_col + mean_sq) * STEP_RATE
    for c in range(chunks):
        cols = slice(c * LANES, (c + 1) * LANES)
        new_ref[:, cols] = table_ref[:, cols] - grads[c] * step


def hot_kernel(got_ref, table_ref, accum_ref, new_ref, new_accum_ref, g_scr):
    n_dev, share, _ = got_ref.shape
    rows, width = table_ref.shape
    chunks = width // LANES
    for g in range(rows // SUBLANES):
        for c in range(chunks):
            first = (g * chunks + c) * SUBLANES
            at = (slice(g * SUBLANES, (g + 1) * SUBLANES), slice(c * LANES, (c + 1) * LANES))
            if share >= SUBLANES:
                g_scr[at] = got_ref[first // share, first % share : first % share + SUBLANES, :]
            else:
                for i in range(SUBLANES):
                    q = first + i
                    g_scr[g * SUBLANES + i : g * SUBLANES + i + 1, at[1]] = got_ref[
                        q // share, q % share : q % share + 1, :
                    ]
    grad = g_scr[...]
    mean_sq = jnp.mean(grad * grad, axis=1, keepdims=True)
    wide = jnp.transpose(jnp.broadcast_to(mean_sq, (rows, LANES)))
    accum_row = accum_ref[...]
    new_accum_ref[...] = accum_row + wide[0:1, :]
    accum_col = jnp.transpose(jnp.broadcast_to(accum_row, (LANES, rows)))[:, 0:1]
    new_ref[...] = table_ref[...] - STEP_RATE * grad * lax.rsqrt(accum_col + mean_sq)


def on_device(
    event_slots,
    fetch_rows,
    fetch_counts,
    hot_table,
    hot_accum,
    cold_table,
    cold_accum,
    ln_gain,
    ln_bias,
    w_in,
    w_out,
    out_grad,
):
    n_rows = lax.axis_size("rows")
    n_rep = lax.axis_size("rep")
    n_dev = n_rows * n_rep
    slot = fetch_rows.shape[1] // n_rows
    hot_rows, width = hot_table.shape
    shard = cold_table.shape[0]
    chunks = width // LANES
    share = hot_rows * chunks // n_dev
    cold_pairs = even(slot * (chunks // n_rep)) // 2
    asks = fetch_rows.shape[1]
    slots = hot_rows + asks

    with jax.named_scope("asks"):
        mine = pl.pallas_call(
            ask_kernel,
            out_shape=pltpu.VMEM((n_dev, 1, asks), jnp.int32),
            in_specs=[ANY],
            out_specs=VMEM,
            scratch_shapes=[pltpu.VMEM((1, asks), jnp.int32), pltpu.SemaphoreType.DMA],
            compiler_params=params(),
            cost_estimate=LONG,
            name="ask",
        )(pltpu.with_memory_space_constraint(fetch_rows, pltpu.HBM))
        asked = lax.all_to_all(mine, ALL, 0, 0, tiled=True)
    found = pl.pallas_call(
        functools.partial(gather_kernel, n_rows=n_rows, n_rep=n_rep, slot=slot),
        out_shape=jax.ShapeDtypeStruct((n_rows, slot * chunks, LANES), F32),
        in_specs=[VMEM, VMEM],
        out_specs=VMEM,
        scratch_shapes=[pltpu.VMEM((n_rows, asks), jnp.int32)],
        compiler_params=params(),
        cost_estimate=LONG,
        name="gather",
    )(asked, cold_table)
    fetched = lax.all_to_all(found, "rows", 0, 0, tiled=True)

    sent = pl.pallas_call(
        functools.partial(layer_kernel, n_dev=n_dev, n_rep=n_rep, slot=slot),
        out_shape=jax.ShapeDtypeStruct((n_dev, even(share) // 2 + cold_pairs, 2, LANES), F32),
        in_specs=[VMEM] * 9,
        out_specs=VMEM,
        scratch_shapes=[
            pltpu.VMEM((slots, width), F32),
            pltpu.VMEM((hot_rows, width), F32),
            pltpu.VMEM((asks, width), F32),
        ],
        compiler_params=params(),
        name="layer",
    )(
        event_slots,
        fetch_counts,
        hot_table,
        fetched,
        ln_gain.reshape(1, width),
        ln_bias.reshape(1, width),
        w_in,
        w_out,
        out_grad,
    )
    got = lax.all_to_all(sent, ALL, 0, 0, tiled=True)

    summed, cold_part = pl.pallas_call(
        sum_kernel,
        out_shape=(
            pltpu.VMEM((n_dev, share, LANES), F32),
            pltpu.VMEM((n_dev, cold_pairs, 2, LANES), F32),
        ),
        in_specs=[VMEM],
        out_specs=(VMEM, VMEM),
        compiler_params=params(),
        name="sum",
    )(got)
    hot_grad = lax.all_to_all(summed, ALL, 0, 0, tiled=True)
    parts = [cold_part] + [
        lax.ppermute(cold_part, "rep", [(i, (i + s) % n_rep) for i in range(n_rep)])
        for s in range(1, n_rep)
    ]

    new_cold_table, new_cold_accum = pl.pallas_call(
        functools.partial(cold_kernel, slot=slot, n_rep=n_rep),
        out_shape=(
            jax.ShapeDtypeStruct((shard, width), F32),
            jax.ShapeDtypeStruct((1, shard), F32),
        ),
        in_specs=[VMEM] * (n_rep + 3),
        out_specs=(VMEM, VMEM),
        scratch_shapes=[pltpu.VMEM((n_rep, n_dev, cold_pairs, 2, LANES), F32)],
        compiler_params=params(),
        name="cold",
    )(asked, *parts, cold_table, cold_accum.reshape(1, shard))

    new_hot_table, new_hot_accum = pl.pallas_call(
        hot_kernel,
        out_shape=(
            jax.ShapeDtypeStruct((hot_rows, width), F32),
            jax.ShapeDtypeStruct((1, hot_rows), F32),
        ),
        in_specs=[VMEM] * 3,
        out_specs=(VMEM, VMEM),
        scratch_shapes=[pltpu.VMEM((hot_rows, width), F32)],
        compiler_params=params(),
        name="hot",
    )(hot_grad, hot_table, hot_accum.reshape(1, hot_rows))
    return (
        new_hot_table,
        new_hot_accum.reshape(hot_rows),
        new_cold_table,
        new_cold_accum.reshape(shard),
    )


def solution(mesh):
    return jax.shard_map(
        on_device,
        mesh=mesh,
        in_specs=(
            P(ALL, None),
            P(ALL, None),
            P(ALL, None),
            P(),
            P(),
            P("rows", None),
            P("rows"),
            P(),
            P(),
            P(),
            P(),
            P(ALL, None),
        ),
        out_specs=(P(), P(), P("rows", None), P("rows")),
        check_vma=False,
    )
```

```python
import functools

import jax
import jax.numpy as jnp
from jax import lax
from jax.experimental import pallas as pl
from jax.experimental.pallas import tpu as pltpu
from jax.sharding import PartitionSpec as P


HEAD = 128
STEP_RATE = 0.5
LANES = 128
SUBLANES = 8
PAIR = 2
REP = ("far", "near")
ALL = ("rows",) + REP
F32 = jnp.float32
BF16 = jnp.bfloat16

LONG = pl.CostEstimate(flops=10**10, bytes_accessed=16 << 20, transcendentals=0)

VMEM = pl.BlockSpec(memory_space=pltpu.VMEM)
ANY = pl.BlockSpec(memory_space=pl.ANY)


def params(mib=24):
    return pltpu.CompilerParams(vmem_limit_bytes=mib << 20)


def dot(a, b, dims, precision=None):
    return lax.dot_general(
        a, b, (dims, ((), ())), preferred_element_type=F32, precision=precision
    )


NN = ((1,), (0,))
NT = ((1,), (1,))
TN = ((0,), (0,))


def rep_index():
    return lax.axis_index("far") * PAIR + lax.axis_index("near")


def ask_kernel(rows_hbm, out_ref, rows_scr, sem):
    copy = pltpu.make_async_copy(rows_hbm, rows_scr, sem)
    copy.start()
    copy.wait()
    out_ref[...] = jnp.broadcast_to(rows_scr[...][None], out_ref.shape)


def even(n):
    return n + n % 2


def gather_kernel(asked_ref, table_ref, out_ref, *, n_rep, slot):
    j = lax.axis_index("rows")
    p = rep_index()
    n_dev = asked_ref.shape[0]
    shard, width = table_ref.shape
    part = width // LANES // n_rep

    asked = asked_ref[:, 0, :]
    pos = lax.broadcasted_iota(jnp.int32, asked.shape, 1)
    picks = []
    for k in range(slot):
        col = jnp.sum(jnp.where(pos == j * slot + k, asked, 0), axis=1, keepdims=True)
        picks.append((lax.broadcasted_iota(jnp.int32, (n_dev, shard), 1) == col).astype(F32))
    pick = jnp.concatenate(picks, axis=0).astype(BF16)
    for c in range(part):
        first = pl.multiple_of((p * part + c) * LANES, LANES)
        table = table_ref[:, pl.ds(first, LANES)]
        high = table.astype(BF16)
        rest = table - high.astype(F32)
        mid = rest.astype(BF16)
        low = (rest - mid.astype(F32)).astype(BF16)
        rows = dot(pick, high, NN) + dot(pick, mid, NN) + dot(pick, low, NN)
        for k in range(slot):
            off = k * part + c
            out_ref[:, off // 2, off % 2, :] = rows[k * n_dev : (k + 1) * n_dev, :]


def normalise(x, eps):
    cent = x - jnp.mean(x, axis=1, keepdims=True)
    rstd = lax.rsqrt(jnp.mean(cent * cent, axis=1, keepdims=True) + eps)
    return cent * rstd, rstd


def project(x_hat, gain, bias, w_in):
    pre = dot((x_hat * gain + bias).astype(BF16), w_in, NN)
    sig = jax.nn.sigmoid(pre)
    return (pre * sig).astype(BF16), sig * (1.0 + pre * (1.0 - sig))


def layer_kernel(
    event_ref,
    count_ref,
    hot_ref,
    fetched_ref,
    gain_ref,
    bias_ref,
    w_in_ref,
    w_out_ref,
    grad_ref,
    *refs,
    n_dev,
    n_rep,
    slot,
    share,
    paired,
):
    out_ref = refs[0]
    x_scr, c_scr, hot_scr, cold_scr = refs[-4:]
    hot_rows, width = hot_ref.shape
    n_owner = n_dev // n_rep
    chunks = width // LANES
    part = chunks // n_rep
    slots = x_scr.shape[0]
    fetched = slots - hot_rows
    seq = grad_ref.shape[0]
    inner = w_out_ref.shape[0]
    heads = inner // HEAD
    gain = gain_ref[...]

    owner = lax.broadcasted_iota(jnp.int32, (fetched, n_owner), 0) // slot
    mine = owner == lax.broadcasted_iota(jnp.int32, (fetched, n_owner), 1)
    counts = jnp.broadcast_to(count_ref[...], (fetched, n_owner))
    count_col = jnp.sum(jnp.where(mine, counts, 0), axis=1, keepdims=True)
    live = (lax.broadcasted_iota(jnp.int32, (fetched, 1), 0) % slot < count_col).astype(F32)

    for j in range(n_owner):
        for c in range(chunks):
            cols = slice(c * LANES, (c + 1) * LANES)
            frm = j * n_rep + c // part
            if part == 1 and slot == 2:
                c_scr[j * slot : (j + 1) * slot, cols] = fetched_ref[frm, 0]
            else:
                for k in range(slot):
                    off = k * part + c % part
                    at = j * slot + k
                    c_scr[at : at + 1, cols] = fetched_ref[frm, off // 2, off % 2 : off % 2 + 1, :]
    x_scr[0:hot_rows, :] = hot_ref[...]
    x_scr[hot_rows:slots, :] = c_scr[...] * live
    x_hat, rstd = normalise(x_scr[...], 1e-05)
    proj, dsilu = project(x_hat, gain, bias_ref[...], w_in_ref[...])

    scatter = (
        lax.broadcasted_iota(jnp.int32, (slots, seq), 0)
        == jnp.broadcast_to(event_ref[...], (slots, seq))
    ).astype(F32)
    scatter_b = scatter.astype(BF16)
    proj_ev = dot(scatter_b, proj, TN).astype(BF16)
    gates = proj_ev[:, 0:inner].astype(F32)

    scale = HEAD ** (-0.5)
    causal = (
        lax.broadcasted_iota(jnp.int32, (seq, seq), 0)
        >= lax.broadcasted_iota(jnp.int32, (seq, seq), 1)
    ).astype(F32) * (1.0 / seq)

    values, queries, keys, atts, dacts, mixeds = [], [], [], [], [], []
    for h in range(heads):
        lo = h * HEAD
        v = proj_ev[:, inner + lo : inner + lo + HEAD]
        q = proj_ev[:, 2 * inner + lo : 2 * inner + lo + HEAD]
        kk = proj_ev[:, 3 * inner + lo : 3 * inner + lo + HEAD]
        s = dot(q, kk, NT) * scale
        sg = jax.nn.sigmoid(s)
        a = (s * sg * causal).astype(BF16)
        dacts.append(sg * (1.0 + s * (1.0 - sg)) * causal)
        values.append(v)
        queries.append(q)
        keys.append(kk)
        atts.append(a)
        mixeds.append(dot(a, v, NN))
    y, mrstd = normalise(jnp.concatenate(mixeds, axis=1), 1e-06)

    grad = grad_ref[...]
    d_gated = dot(grad, w_out_ref[...], NT).astype(BF16).astype(F32)
    d_gates = (d_gated * y).astype(BF16)
    d_y = d_gated * gates
    d_mixed = mrstd * (
        d_y - jnp.mean(d_y, axis=1, keepdims=True) - y * jnp.mean(d_y * y, axis=1, keepdims=True)
    )
    d_mixed = d_mixed.astype(BF16)
    d_vs, d_qs, d_ks = [], [], []
    for h in range(heads):
        dm = d_mixed[:, h * HEAD : (h + 1) * HEAD]
        d_a = dot(dm, values[h], NT).astype(BF16).astype(F32)
        d_vs.append(dot(atts[h], dm, TN).astype(BF16))
        d_s = (d_a * dacts[h] * scale).astype(BF16)
        d_qs.append(dot(d_s, keys[h], NN).astype(BF16))
        d_ks.append(dot(d_s, queries[h], TN).astype(BF16))
    d_proj = jnp.concatenate([d_gates] + d_vs + d_qs + d_ks, axis=1)

    d_slot = dot(scatter_b, d_proj, NN)
    d_hat = dot((d_slot * dsilu).astype(BF16), w_in_ref[...], NT) * gain
    d_x = rstd * (
        d_hat
        - jnp.mean(d_hat, axis=1, keepdims=True)
        - x_hat * jnp.mean(d_hat * x_hat, axis=1, keepdims=True)
    )
    d_x = d_x + dot(scatter_b, grad, NN)
    for c in range(chunks):
        cols = slice(c * LANES, (c + 1) * LANES)
        hot_scr[c] = d_x[0:hot_rows, cols]
        cold_scr[c] = d_x[hot_rows:slots, cols] * live

    near = lax.axis_index("near")
    if paired:
        tiles = share // SUBLANES
        half = tiles // PAIR
        base = half * SUBLANES // 2
        for to_ref, side in ((out_ref, near), (refs[1], 1 - near)):
            for d in range(n_dev):
                g, c = divmod(d * tiles, chunks)
                for i in range(half):
                    tile = hot_scr[c + side * half + i, g * SUBLANES : (g + 1) * SUBLANES, :]
                    to_ref[d, i * SUBLANES // 2 : (i + 1) * SUBLANES // 2] = tile.reshape(
                        SUBLANES // 2, 2, LANES
                    )
    else:
        base = even(share) // 2
        for row in range(hot_rows):
            for c in range(chunks):
                unit = (row // SUBLANES * chunks + c) * SUBLANES + row % SUBLANES
                to, off = divmod(unit, share)
                out_ref[to, off // 2, off % 2 : off % 2 + 1, :] = hot_scr[c, row : row + 1, :]

    for j in range(n_owner):
        for c in range(chunks):
            to = j * n_rep + c // part
            if part == 1 and slot == 2:
                out_ref[to, base] = cold_scr[c, j * slot : (j + 1) * slot, :]
            else:
                for k in range(slot):
                    off = k * part + c % part
                    at = j * slot + k
                    out_ref[to, base + off // 2, off % 2 : off % 2 + 1, :] = cold_scr[c, at : at + 1, :]


def pair_kernel(keep_ref, got_ref, out_ref):
    base = got_ref.shape[1]
    out_ref[:, 0:base] = keep_ref[:, 0:base] + got_ref[...]
    out_ref[:, base:] = keep_ref[:, base:]


def sum_kernel(got_ref, out_ref, cold_ref, *, base, sides):
    n_dev = got_ref.shape[0]
    share = out_ref.shape[1]
    for side in range(sides):
        total = got_ref[side, 0:base]
        for d in range(side + sides, n_dev, sides):
            total = total + got_ref[d, 0:base]
        total = total.reshape(2 * base, LANES)[0:share]
        for d in range(side, n_dev, sides):
            out_ref[d] = total
    cold_ref[...] = got_ref[:, base:]


def cold_kernel(asked_ref, *refs, slot, n_rep):
    part_refs = refs[:n_rep]
    table_ref, accum_ref, new_ref, new_accum_ref, part_scr = refs[n_rep:]
    j = lax.axis_index("rows")
    p = rep_index()
    n_dev = asked_ref.shape[0]
    shard, width = table_ref.shape
    chunks = width // LANES
    part = chunks // n_rep
    for s in range(n_rep):
        part_scr[(p + n_rep - s) % n_rep] = part_refs[s][...]
    asked = asked_ref[:, 0, :]
    pos = lax.broadcasted_iota(jnp.int32, asked.shape, 1)
    picks = []
    for k in range(slot):
        col = jnp.sum(jnp.where(pos == j * slot + k, asked, 0), axis=1, keepdims=True)
        picks.append((lax.broadcasted_iota(jnp.int32, (n_dev, shard), 1) == col).astype(F32))
    pick = jnp.concatenate(picks, axis=0)
    grads = []
    for c in range(chunks):
        rows = []
        for k in range(slot):
            off = k * part + c % part
            rows.append(part_scr[c // part, :, off // 2, off % 2, :])
        grads.append(dot(pick, jnp.concatenate(rows, axis=0), TN, lax.Precision.HIGHEST))
    total = grads[0] * grads[0]
    for g in grads[1:]:
        total = total + g * g
    mean_sq = jnp.sum(total, axis=1, keepdims=True) * (1.0 / width)
    wide = jnp.transpose(jnp.broadcast_to(mean_sq, (shard, LANES)))
    accum_row = accum_ref[...]
    new_accum_ref[...] = accum_row + wide[0:1, :]
    accum_col = jnp.transpose(jnp.broadcast_to(accum_row, (LANES, shard)))[:, 0:1]
    step = lax.rsqrt(accum_col + mean_sq) * STEP_RATE
    for c in range(chunks):
        cols = slice(c * LANES, (c + 1) * LANES)
        new_ref[:, cols] = table_ref[:, cols] - grads[c] * step


def hot_kernel(*refs, paired):
    n_in = 1 + paired
    table_ref, accum_ref, new_ref, new_accum_ref, g_scr = refs[n_in : n_in + 5]
    rows, width = table_ref.shape
    chunks = width // LANES
    if paired:
        own_ref, twin_ref, got_ref = refs[0], refs[1], refs[-1]
        near = lax.axis_index("near")
        got_ref[near] = own_ref[...]
        got_ref[1 - near] = twin_ref[...]
        half = own_ref.shape[1] // SUBLANES
        for tile in range(rows // SUBLANES * chunks):
            g, c = divmod(tile, chunks)
            d, i = divmod(tile, PAIR * half)
            off = i % half * SUBLANES
            g_scr[g * SUBLANES : (g + 1) * SUBLANES, c * LANES : (c + 1) * LANES] = got_ref[
                i // half, d, off : off + SUBLANES, :
            ]
    else:
        share = refs[0].shape[1]
        for row in range(rows):
            for c in range(chunks):
                unit = (row // SUBLANES * chunks + c) * SUBLANES + row % SUBLANES
                frm, off = divmod(unit, share)
                g_scr[row : row + 1, c * LANES : (c + 1) * LANES] = refs[0][frm, off : off + 1, :]
    grad = g_scr[...]
    mean_sq = jnp.mean(grad * grad, axis=1, keepdims=True)
    wide = jnp.transpose(jnp.broadcast_to(mean_sq, (rows, LANES)))
    accum_row = accum_ref[...]
    new_accum_ref[...] = accum_row + wide[0:1, :]
    accum_col = jnp.transpose(jnp.broadcast_to(accum_row, (LANES, rows)))[:, 0:1]
    new_ref[...] = table_ref[...] - STEP_RATE * grad * lax.rsqrt(accum_col + mean_sq)


def on_device(
    event_slots,
    fetch_rows,
    fetch_counts,
    hot_table,
    hot_accum,
    cold_table,
    cold_accum,
    ln_gain,
    ln_bias,
    w_in,
    w_out,
    out_grad,
):
    n_rows = lax.axis_size("rows")
    n_rep = lax.axis_size("far") * PAIR
    n_dev = n_rows * n_rep
    slot = fetch_rows.shape[1] // n_rows
    hot_rows, width = hot_table.shape
    shard = cold_table.shape[0]
    chunks = width // LANES
    share = hot_rows * chunks // n_dev
    tiles = share // SUBLANES
    paired = share % (PAIR * SUBLANES) == 0 and chunks % max(tiles, 1) == 0
    sides = PAIR if paired else 1
    unit = share // sides
    base = even(unit) // 2
    cold_pairs = even(slot * (chunks // n_rep)) // 2
    asks = fetch_rows.shape[1]
    slots = hot_rows + asks

    mine = pl.pallas_call(
        ask_kernel,
        out_shape=pltpu.VMEM((n_dev, 1, asks), jnp.int32),
        in_specs=[ANY],
        out_specs=VMEM,
        scratch_shapes=[pltpu.VMEM((1, asks), jnp.int32), pltpu.SemaphoreType.DMA],
        compiler_params=params(),
        cost_estimate=LONG,
        name="ask",
    )(pltpu.with_memory_space_constraint(fetch_rows, pltpu.HBM))
    asked = lax.all_to_all(mine, ALL, 0, 0, tiled=True)
    found = pl.pallas_call(
        functools.partial(gather_kernel, n_rep=n_rep, slot=slot),
        out_shape=jax.ShapeDtypeStruct((n_dev, cold_pairs, 2, LANES), F32),
        in_specs=[VMEM, VMEM],
        out_specs=VMEM,
        compiler_params=params(),
        cost_estimate=LONG,
        name="gather",
    )(asked, cold_table)
    fetched = lax.all_to_all(found, ALL, 0, 0, tiled=True)

    out = [(n_dev, base + cold_pairs, 2, LANES)] + [(n_dev, base, 2, LANES)] * paired
    sent = pl.pallas_call(
        functools.partial(
            layer_kernel, n_dev=n_dev, n_rep=n_rep, slot=slot, share=share, paired=paired
        ),
        out_shape=[jax.ShapeDtypeStruct(x, F32) for x in out],
        in_specs=[VMEM] * 9,
        out_specs=[VMEM] * len(out),
        scratch_shapes=[
            pltpu.VMEM((slots, width), F32),
            pltpu.VMEM((asks, width), F32),
            pltpu.VMEM((chunks, hot_rows, LANES), F32),
            pltpu.VMEM((chunks, asks, LANES), F32),
        ],
        compiler_params=params(),
        name="layer",
    )(
        event_slots,
        fetch_counts,
        hot_table,
        fetched,
        ln_gain.reshape(1, width),
        ln_bias.reshape(1, width),
        w_in,
        w_out,
        out_grad,
    )
    swap = [(i, 1 - i) for i in range(PAIR)]
    both = sent[0]
    if paired:
        both = pl.pallas_call(
            pair_kernel,
            out_shape=jax.ShapeDtypeStruct(out[0], F32),
            in_specs=[VMEM] * 2,
            out_specs=VMEM,
            compiler_params=params(),
            name="pair",
        )(both, lax.ppermute(sent[1], "near", swap))
    got = lax.all_to_all(both, ALL, 0, 0, tiled=True)

    summed, cold_part = pl.pallas_call(
        functools.partial(sum_kernel, base=base, sides=sides),
        out_shape=(
            pltpu.VMEM((n_dev, unit, LANES), F32),
            pltpu.VMEM((n_dev, cold_pairs, 2, LANES), F32),
        ),
        in_specs=[VMEM],
        out_specs=(VMEM, VMEM),
        compiler_params=params(),
        name="sum",
    )(got)
    own = lax.all_to_all(summed, ALL, 0, 0, tiled=True)
    grads = [own] + [lax.ppermute(own, "near", swap)] * paired
    parts = [cold_part] + [
        lax.ppermute(cold_part, REP, [(i, (i + s) % n_rep) for i in range(n_rep)])
        for s in range(1, n_rep)
    ]
    new_cold_table, new_cold_accum = pl.pallas_call(
        functools.partial(cold_kernel, slot=slot, n_rep=n_rep),
        out_shape=(
            jax.ShapeDtypeStruct((shard, width), F32),
            jax.ShapeDtypeStruct((1, shard), F32),
        ),
        in_specs=[VMEM] * (n_rep + 3),
        out_specs=(VMEM, VMEM),
        scratch_shapes=[pltpu.VMEM((n_rep, n_dev, cold_pairs, 2, LANES), F32)],
        compiler_params=params(),
        name="cold",
    )(asked, *parts, cold_table, cold_accum.reshape(1, shard))

    new_hot_table, new_hot_accum = pl.pallas_call(
        functools.partial(hot_kernel, paired=paired),
        out_shape=(
            jax.ShapeDtypeStruct((hot_rows, width), F32),
            jax.ShapeDtypeStruct((1, hot_rows), F32),
        ),
        in_specs=[VMEM] * (len(grads) + 2),
        out_specs=(VMEM, VMEM),
        scratch_shapes=[pltpu.VMEM((hot_rows, width), F32)]
        + [pltpu.VMEM((PAIR, n_dev, unit, LANES), F32)] * paired,
        compiler_params=params(),
        name="hot",
    )(*grads, hot_table, hot_accum.reshape(1, hot_rows))
    return (
        new_hot_table,
        new_hot_accum.reshape(hot_rows),
        new_cold_table,
        new_cold_accum.reshape(shard),
    )


def solution(mesh):
    n_rows, n_rep = mesh.shape["rows"], mesh.shape["rep"]
    devices = mesh.devices.reshape(n_rows, n_rep // PAIR, PAIR)
    return jax.shard_map(
        on_device,
        mesh=jax.sharding.Mesh(devices, ALL),
        in_specs=(
            P(ALL, None),
            P(ALL, None),
            P(ALL, None),
            P(),
            P(),
            P("rows", None),
            P("rows"),
            P(),
            P(),
            P(),
            P(),
            P(ALL, None),
        ),
        out_specs=(P(), P(), P("rows", None), P("rows")),
        check_vma=False,
    )
```
